32 devices in a mesh: rows: 4 (over z), cols: 4 (over y, x), space: 2 (over core).
Axes of the slice: x: 2, y: 2, z: 4, core: 2. Of those that a mesh axis runs over, the one named last changes fastest.
Arguments:
- hamiltonian: float32 [2048, 1536], P(('rows', 'cols', 'space')), may hold values from -1 to 1
- correlation_root: float32 [2048, 1536], P('rows'), may hold values from -1 to 2
- pattern: int32 [64, 48], replicated, may hold values from 0 to 1
- sub_blocks: int32 [64, 16], P(('rows', 'cols', 'space')), may hold values from 0 to 47, as said below
- sub_count: int32 [64], P(('rows', 'cols', 'space')), may hold values from 8 to 16, as said below
Outputs:
- density: float32 [2048, 1536], P(('rows', 'cols', 'space'))
- charges: float32 [2048], P(('rows', 'cols', 'space'))
The draws below stay inside these ranges and needn't reach their ends.
Inputs may be any that keep to these rules, and one draw needn't show every extreme that they name: `sub_blocks`: row g lists distinct positions; its first entry is 16 + g mod 16, the position of block g itself. `sub_count`: some submatrix has exactly 16 live blocks.
All inputs are finite; a program needn't handle non-finite values.
Results may differ from the reference program's by a relative error of at most 0.0003.
Values sent between devices are 32-bit elements; how exact they have to be, the bound alone decides.
A program may use at most 128 MiB of HBM per device.

```python
import math
import jax
import jax.numpy as jnp
from jax import lax

BLK = 32
MAXB = 16
NPG = 16
SLAB = 512
WIN = 1536
WB = 48
NB = 64
N = 2048
N_ROWS = 4


def draw_hamiltonian(key, part):
    values = jnp.clip(jax.random.normal(key, (N, WIN), jnp.float32), -6.0, 6.0)
    return values / math.sqrt(WIN)


def draw_correlation_root(key, part):
    entries = jnp.clip(jax.random.normal(key, (N, WIN), jnp.float32), -6.0, 6.0)
    entries = entries * (0.6 / math.sqrt(WIN))
    row_ids = jnp.arange(N, dtype=jnp.int32)
    column_ids = jnp.arange(WIN, dtype=jnp.int32)
    diagonal = (column_ids[None, :] == SLAB + (row_ids % SLAB)[:, None]).astype(jnp.float32)
    return entries + diagonal


def draw_pattern(key, part):
    picks = jax.random.randint(key, (NB, WB), 0, 5)
    block_ids = jnp.arange(NB, dtype=jnp.int32)
    band_ids = jnp.arange(WB, dtype=jnp.int32)
    diagonal = band_ids[None, :] == NPG + (block_ids % NPG)[:, None]
    return jnp.where(diagonal | (picks < 3), 1, 0).astype(jnp.int32)


def draw_sub_blocks(key, part):
    key_list = jax.random.split(jax.random.fold_in(key, 11), NB)
    shuffled = jax.vmap(lambda single: jax.random.permutation(single, WB - 1))(key_list).astype(jnp.int32)
    home_slot = (NPG + jnp.arange(NB, dtype=jnp.int32) % NPG)[:, None]
    neighbours = shuffled + (shuffled >= home_slot).astype(jnp.int32)
    return jnp.concatenate([home_slot, neighbours[:, :MAXB - 1]], axis=1).astype(jnp.int32)


def draw_sub_count(key, part):
    block_counts = jax.random.randint(jax.random.fold_in(key, 5), (NB,), MAXB // 2, MAXB + 1)
    chosen_block = jax.random.randint(jax.random.fold_in(key, 6), (), 0, NB)
    return jnp.where(jnp.arange(NB, dtype=jnp.int32) == chosen_block, MAXB, block_counts).astype(jnp.int32)


def setup_inputs(seed: int = 0) -> dict:
    arg_keys = jax.random.split(jax.random.key(seed), 6)
    hamiltonian = draw_hamiltonian(jax.random.fold_in(arg_keys[5], 71), 0)
    correlation_root = draw_correlation_root(jax.random.fold_in(arg_keys[5], 71), 0)
    pattern = draw_pattern(jax.random.fold_in(arg_keys[5], 71), 0)
    sub_blocks = draw_sub_blocks(jax.random.fold_in(arg_keys[5], 71), 0)
    sub_count = draw_sub_count(jax.random.fold_in(arg_keys[5], 71), 0)
    return dict(hamiltonian=hamiltonian, correlation_root=correlation_root, pattern=pattern, sub_blocks=sub_blocks, sub_count=sub_count)


highest = lax.Precision.HIGHEST

def multiply(leftside, rightside):
    return jnp.dot(leftside, rightside, precision=highest, preferred_element_type=jnp.float32)

def windows(banded):
    stacked = banded.reshape(N_ROWS, SLAB, WIN)
    above_used = jnp.roll(stacked, 1, axis=0)[:, :, SLAB:]
    below_used = jnp.roll(stacked, -1, axis=0)[:, :, :2 * SLAB]
    zero_block = jnp.zeros((N_ROWS, SLAB, SLAB), jnp.float32)
    top_rows = jnp.concatenate([above_used, zero_block], axis=2)
    bottom = jnp.concatenate([zero_block, below_used], axis=2)
    return jnp.concatenate([top_rows, stacked, bottom], axis=1)

def sandwich_step(leftside, rightside, pattern_mask):
    stacked = leftside.reshape(N_ROWS, SLAB, WIN)
    joined = jnp.einsum('sik,skj->sij', stacked, windows(rightside), precision=highest)
    return pattern_mask * joined.reshape(N, WIN)

def density_rows(local_window, positions, live_count):
    offsets = (positions[:, None] * BLK + jnp.arange(BLK, dtype=jnp.int32)[None, :]).reshape(-1)
    live_cols = jnp.repeat((jnp.arange(MAXB, dtype=jnp.int32) < live_count).astype(jnp.float32), BLK)
    assembled = jnp.take(jnp.take(local_window, offsets, axis=0), offsets, axis=1)
    assembled = assembled * live_cols[:, None] * live_cols[None, :]
    symmetric = 0.5 * (assembled + assembled.T)
    live_order = (live_count * BLK).astype(jnp.float32)
    normalizer = jnp.sqrt(live_order) / (2.0 * jnp.sqrt(jnp.sum(symmetric * symmetric) + 1e-06))
    iterate = symmetric * normalizer
    square = multiply(iterate, iterate)
    iterate = 1.5 * iterate - 0.5 * multiply(iterate, square)
    square = multiply(iterate, iterate)
    home_rows = iterate[:BLK]
    home_rows = 1.5 * home_rows - 0.5 * multiply(home_rows, square)
    padded_order = MAXB * BLK
    home_eye = (jnp.arange(BLK, dtype=jnp.int32)[:, None] == jnp.arange(padded_order, dtype=jnp.int32)[None, :]).astype(jnp.float32)
    home_density = 0.5 * (home_eye - home_rows)
    placement = (offsets[:, None] == jnp.arange(local_window.shape[1], dtype=jnp.int32)[None, :]).astype(jnp.float32)
    return multiply(home_density, placement)

def reference(hamiltonian, correlation_root, pattern, sub_blocks, sub_count):
    pattern_mask = jnp.repeat(jnp.repeat(pattern.astype(jnp.float32), BLK, axis=0), BLK, axis=1)
    half_done = sandwich_step(hamiltonian, correlation_root, pattern_mask)
    orthogonal = sandwich_step(correlation_root, half_done, pattern_mask)
    ortho_windows = windows(orthogonal)

    def solve_block(entries):
        block_index, positions, live_count = entries
        slab_index = (block_index // NPG).astype(jnp.int32)
        local_window = lax.dynamic_index_in_dim(ortho_windows, slab_index, 0, keepdims=False)
        return density_rows(local_window, positions, live_count)
    density_blocks = lax.map(solve_block, (jnp.arange(NB, dtype=jnp.int32), sub_blocks, sub_count))
    density_band = density_blocks.reshape(N, WIN)
    half_back = sandwich_step(density_band, correlation_root, pattern_mask)
    density = sandwich_step(correlation_root, half_back, pattern_mask)
    charges = lax.optimization_barrier(jnp.sum(density, axis=1))
    return (density, charges)
```

```python
import functools

import jax
import jax.numpy as jnp
from jax import lax
from jax.experimental import pallas as pl
from jax.experimental.pallas import tpu as pltpu
from jax.sharding import PartitionSpec as P

BLK = 32
F32 = jnp.float32
BF16 = jnp.bfloat16


def split(value):
    upper = value.astype(BF16)
    return upper, (value - upper.astype(F32)).astype(BF16)


def dot(leftside, rightside):
    return jnp.dot(leftside, rightside, preferred_element_type=F32)


def product(stacked, right):
    high, low = right
    half = stacked.shape[0] // 2
    both = dot(stacked, high)
    return both[:half] + both[half:] + dot(stacked[:half], low)


def stack(value):
    return jnp.concatenate(split(value), axis=0)


def combine(above, own, below, width):
    return jnp.concatenate(
        [
            above[:, :width] + own[:, :width],
            above[:, width:] + own[:, width : 2 * width] + below[:, :width],
            own[:, 2 * width :] + below[:, width:],
        ],
        axis=1,
    )


class Sender:
    def __init__(self, send_sems, recv_sems):
        self.sems = (send_sems, recv_sems)
        self.copies = []

    def __call__(self, source, target, device):
        slot = len(self.copies)
        copy = pltpu.make_async_remote_copy(
            src_ref=source,
            dst_ref=target,
            send_sem=self.sems[0].at[slot],
            recv_sem=self.sems[1].at[slot],
            device_id=device,
            device_id_type=pl.DeviceIdType.MESH,
        )
        copy.start()
        self.copies.append(copy)
        return copy

    def finish(self):
        for copy in self.copies:
            copy.wait_send()


def kernel(
    pos_ref,
    count_ref,
    ham_ref,
    root_ref,
    pattern_ref,
    density_ref,
    charges_ref,
    root_v,
    left_s,
    ham_v,
    land_v,
    wide_hi,
    wide_lo,
    near_hi,
    near_lo,
    mask_a,
    mask_b,
    half_v,
    back_v,
    ortho_v,
    acc_v,
    sub_v,
    band_v,
    rows_v,
    strip_v,
    final_v,
    local_sems,
    send_sems,
    recv_sems,
):
    row = lax.axis_index("rows")
    count = lax.axis_size("rows")
    col = lax.axis_index("cols")
    space = lax.axis_index("space")
    cols = lax.axis_size("cols")
    slab, window = root_v.shape
    own = ham_ref.shape[0]
    chunk = slab // cols
    half = slab // 2
    maxb = pos_ref.shape[1]
    slab_blocks = slab // BLK
    own_blocks = own // BLK
    order = maxb * BLK
    groups = chunk // BLK

    first = col + 1 - 2 * lax.rem(col, 2)
    second = lax.rem(col + 2, 4)
    third = lax.rem(first + 2, 4)
    above = lax.rem(row + 1, count)
    below = lax.rem(row + count - 1, count)
    up, down = {"rows": above}, {"rows": below}
    side, cross, mate = {"cols": first}, {"cols": second}, {"space": 1 - space}
    lanes = pl.ds(pl.multiple_of(chunk * col, chunk), chunk)

    load_root = pltpu.make_async_copy(root_ref, root_v, local_sems.at[0])
    load_ham = pltpu.make_async_copy(ham_ref, ham_v.at[col], local_sems.at[1])
    load_root.start()
    load_ham.start()

    barrier = pltpu.get_barrier_semaphore()
    peers = [mate]
    for offset in range(cols):
        other = lax.rem(col + offset, cols)
        peers += [{"rows": above, "cols": other}, {"rows": below, "cols": other}]
        if offset:
            peers.append({"cols": other})
    for peer in peers:
        pl.semaphore_signal(barrier, inc=1, device_id=peer, device_id_type=pl.DeviceIdType.MESH)
    pl.semaphore_wait(barrier, len(peers))
    send = Sender(send_sems, recv_sems)

    ham_first = send(ham_ref, ham_v.at[col], side)
    ham_second = send(ham_ref, ham_v.at[col], cross)

    def land(piece, k, part=None):
        size = half if part is None else half // 2
        start = half * space + (0 if part is None else part * size)
        return land_v.at[
            piece // 2,
            piece % 2,
            pl.ds(pl.multiple_of(start, size), size),
            pl.ds(pl.multiple_of(chunk * k, chunk), chunk),
        ]

    order_of_pieces = (0, 2, 1, 3)
    pieces = {}
    for piece in order_of_pieces:
        panel = (1, 2, 1, 0)[piece]
        source = root_ref.at[
            pl.ds(pl.multiple_of(half * space, half), half),
            pl.ds(pl.multiple_of(panel * slab + chunk * col, chunk), chunk),
        ]
        pieces[piece] = send(source, land(piece, col), up if piece < 2 else down)

    zero = jnp.zeros(ortho_v.shape[3:], F32)
    for part in range(2):
        ortho_v[0, 2, part] = zero
        ortho_v[2, 0, part] = zero

    pattern = pattern_ref[...].astype(F32).astype(BF16)
    blocks_all = pattern.shape[0]

    def pick(rows, block_of):
        wanted = block_of(lax.broadcasted_iota(jnp.int32, (rows, blocks_all), 0))
        here = lax.broadcasted_iota(jnp.int32, (rows, blocks_all), 1)
        return dot(jnp.where(wanted == here, 1.0, 0.0).astype(BF16), pattern).astype(BF16)

    def spread(values, wanted):
        here = lax.broadcasted_iota(jnp.int32, wanted.shape, 0)
        return dot(values, jnp.where(wanted == here, 1.0, 0.0).astype(BF16))

    base = row * slab_blocks
    strip_rows = pick(
        cols * own,
        lambda i: base + ((i // own) * 2 + space) * own_blocks + (i % own) // BLK,
    )
    lane = lax.broadcasted_iota(jnp.int32, (3 * slab_blocks, 3 * chunk), 1)
    chip_mask = spread(
        strip_rows, (lane // chunk) * slab_blocks + col * groups + (lane % chunk) // BLK
    )
    for i in range(cols):
        mask_a[i] = chip_mask[i * own : (i + 1) * own]
    own_rows = pick(own, lambda i: base + (col * 2 + space) * own_blocks + i // BLK)
    lane = lax.broadcasted_iota(jnp.int32, (3 * slab_blocks, window), 1)
    mask_b[...] = spread(own_rows, lane // BLK)

    load_root.wait()
    for i in range(cols):
        start = pl.multiple_of((i * 2 + space) * own, own)
        upper, lower = split(root_v[pl.ds(start, own), :])
        left_s[0, i * own : (i + 1) * own] = upper
        left_s[1, i * own : (i + 1) * own] = lower
    for b in range(3):
        wide_hi[1, b], wide_lo[1, b] = split(root_v[:, b * slab : (b + 1) * slab])
        start = pl.multiple_of(b * slab + chunk * col, chunk)
        upper, lower = split(root_v[:, pl.ds(start, chunk)])
        near_hi[1, :, b * chunk : (b + 1) * chunk] = upper
        near_lo[1, :, b * chunk : (b + 1) * chunk] = lower

    relayed = {}
    gathers = {}

    def arrive(piece):
        pieces[piece].wait_recv()
        relayed[piece] = send(land(piece, col), land(piece, col), mate)

    def offer(piece):
        gathers[piece] = [
            send(land(piece, col), land(piece, col), side),
            send(land(piece, col), land(piece, col), cross),
        ]

    def half_rows(k, part):
        return ham_v.at[k, pl.ds(part * (own // 2), own // 2), :]

    arrive(0)
    arrive(2)
    ham_first.wait_recv()
    ham_half_a = send(half_rows(first, 1), half_rows(first, 1), cross)
    ham_second.wait_recv()
    ham_half_b = send(half_rows(second, 0), half_rows(second, 0), side)
    offer(0)
    offer(2)
    arrive(1)
    arrive(3)
    offer(1)
    offer(3)
    for piece in order_of_pieces:
        relayed[piece].wait_recv()
        upper, lower = split(land_v[piece // 2, piece % 2, :, lanes])
        side_of = 0 if piece < 2 else 2
        place = (0, 1, 1, 0)[piece]
        near_hi[side_of, :, place * chunk : (place + 1) * chunk] = upper
        near_lo[side_of, :, place * chunk : (place + 1) * chunk] = lower

    load_ham.wait()
    strips = (col, first, second, third)
    half_up, half_down, half_mate = [], [], []
    for i, strip in enumerate(strips):
        if i == 3:
            ham_half_a.wait_recv()
            ham_half_b.wait_recv()
        stacked = stack(ham_v[strip])
        terms = []
        for a in range(3):
            width = 3 * chunk if a == 1 else 2 * chunk
            terms.append(
                product(
                    stacked[:, a * slab : (a + 1) * slab],
                    (near_hi[a, :, :width], near_lo[a, :, :width]),
                )
            )
        done = mask_a[strip] * combine(*terms, chunk)
        for b in range(3):
            half_v[1, b, strip, space] = done[:, b * chunk : (b + 1) * chunk]
        half_up.append(
            send(
                half_v.at[1, pl.ds(1, 2), strip, space],
                half_v.at[0, pl.ds(0, 2), strip, space],
                up,
            )
        )
        half_down.append(
            send(
                half_v.at[1, pl.ds(0, 2), strip, space],
                half_v.at[2, pl.ds(1, 2), strip, space],
                down,
            )
        )
        half_mate.append(
            send(half_v.at[1, :, strip, space], half_v.at[1, :, strip, space], mate)
        )

    def window_block(ref, a):
        picked = {0: (0, 1), 1: (0, 1, 2), 2: (1, 2)}[a]
        return split(
            jnp.concatenate([ref[a, b].reshape(slab, chunk) for b in picked], axis=1)
        )

    def left_block(a):
        return left_s[:, :, a * slab : (a + 1) * slab].reshape(2 * half, slab)

    for copy in half_mate:
        copy.wait_recv()
    acc_v[...] = product(left_block(1), window_block(half_v, 1))
    relays = []
    mates = []
    for i, piece in enumerate(order_of_pieces):
        gathers[piece][0].wait_recv()
        relays.append(send(land(piece, first, 1), land(piece, first, 1), cross))
        mates.append(send(land(piece, first), land(piece, first), mate))
        gathers[piece][1].wait_recv()
        relays.append(send(land(piece, second, 0), land(piece, second, 0), side))
        mates.append(send(land(piece, second), land(piece, second), mate))
        half_up[i].wait_recv()
        region = half_v.at[0, pl.ds(0, 2), strips[i], space]
        half_mate.append(send(region, region, mate))
        half_down[i].wait_recv()
        region = half_v.at[2, pl.ds(1, 2), strips[i], space]
        half_mate.append(send(region, region, mate))
    for copy in half_mate[cols:]:
        copy.wait_recv()

    done = combine(
        product(left_block(0), window_block(half_v, 0)),
        acc_v[...],
        product(left_block(2), window_block(half_v, 2)),
        chunk,
    )
    for b in range(3):
        masked = mask_a[:, :, b * chunk : (b + 1) * chunk].reshape(half, chunk)
        masked = masked * done[:, b * chunk : (b + 1) * chunk]
        ortho_v[1, b, space, :, col] = masked.reshape(half // BLK, BLK, chunk)

    spans = {0: (0, 2), 1: (0, 3), 2: (1, 2)}

    def region(a, k, part=None, span=None):
        size = half // BLK if part is None else half // BLK // 2
        start = 0 if part is None else part * size
        return ortho_v.at[a, pl.ds(*(span or spans[a])), space, pl.ds(start, size), k]

    def pass_on(a, k, part, device):
        return send(region(a, k, part), region(a, k, part), device)

    def to_rows(k, part):
        return (
            send(region(1, k, part, (1, 2)), region(0, k, part), up),
            send(region(1, k, part, (0, 2)), region(2, k, part), down),
        )

    pending = []
    own_rows_out = to_rows(col, None)
    own_first = pass_on(1, col, None, side)
    own_second = pass_on(1, col, None, cross)
    pending.append(pass_on(1, col, None, mate))
    for copy in relays:
        copy.wait_recv()
    for piece in order_of_pieces:
        mates.append(send(land(piece, third), land(piece, third), mate))
    for copy in mates:
        copy.wait_recv()
    for piece in order_of_pieces:
        a = 0 if piece < 2 else 2
        b = (0, 1, 2, 1)[piece]
        wide_hi[a, b], wide_lo[a, b] = split(land_v[piece // 2, piece % 2])

    own_first.wait_recv()
    diagonal_a = pass_on(1, first, 1, cross)
    first_rows = to_rows(first, 0)
    pending.append(pass_on(1, first, None, mate))
    own_second.wait_recv()
    diagonal_b = pass_on(1, second, 0, side)
    second_rows = to_rows(second, 1)
    pending.append(pass_on(1, second, None, mate))
    hops = []
    for a, copy in ((0, own_rows_out[0]), (2, own_rows_out[1])):
        copy.wait_recv()
        hops.append((a, first, 1, pass_on(a, col, 1, side)))
        hops.append((a, second, 0, pass_on(a, col, 0, cross)))
        pending.append(pass_on(a, col, None, mate))
    diagonal_a.wait_recv()
    diagonal_b.wait_recv()
    pending.append(pass_on(1, third, None, mate))
    for a, copy in ((0, first_rows[0]), (2, first_rows[1])):
        copy.wait_recv()
        hops.append((a, third, 0, pass_on(a, first, 0, cross)))
        pending.append(pass_on(a, first, 0, mate))
    for a, copy in ((0, second_rows[0]), (2, second_rows[1])):
        copy.wait_recv()
        hops.append((a, third, 1, pass_on(a, second, 1, side)))
        pending.append(pass_on(a, second, 1, mate))
    for a, k, part, copy in hops:
        copy.wait_recv()
        pending.append(pass_on(a, k, part, mate))
    for copy in pending:
        copy.wait_recv()

    lane_group = lax.broadcasted_iota(jnp.int32, (BLK, chunk), 1) // BLK

    def turn(value, steps):
        steps = jnp.full((BLK, chunk), steps, jnp.int32)
        step = 1
        while step < groups:
            moved = pltpu.roll(value, step * BLK, 1)
            value = jnp.where(steps & step == step, moved, value)
            step *= 2
        return value

    def solve(g, carry):
        live = count_ref[g]

        def assemble(i, inner):
            block = pos_ref[g, i]
            a = lax.div(block, slab_blocks)
            within = lax.rem(block, slab_blocks)
            owner = lax.div(within, own_blocks)
            core = lax.rem(owner, 2)
            place = lax.div(owner, 2) * own_blocks + lax.rem(within, own_blocks)
            for t in range(maxb // groups):
                tile = jnp.zeros((BLK, chunk), F32)
                for e in range(groups):
                    other = pos_ref[g, t * groups + e]
                    b = lax.div(other, slab_blocks)
                    inside = lax.rem(other, slab_blocks)
                    value = ortho_v[a, b, core, place, lax.div(inside, groups)]
                    value = turn(value, lax.rem(e + groups - lax.rem(inside, groups), groups))
                    tile = jnp.where(lane_group == e, value, tile)
                sub_v[pl.ds(pl.multiple_of(i * BLK, BLK), BLK), t * chunk : (t + 1) * chunk] = tile
            return inner

        lax.fori_loop(0, maxb, assemble, 0)
        position = [lax.broadcasted_iota(jnp.int32, (order, order), d) for d in range(2)]
        assembled = jnp.where(jnp.maximum(*position) < live * BLK, sub_v[...], 0.0)
        symmetric = 0.5 * (assembled + assembled.T)
        total = jnp.sum(jnp.sum(symmetric * symmetric, axis=1, keepdims=True), axis=0, keepdims=True)
        live_order = jnp.full((1, 1), live * BLK, jnp.int32).astype(F32)
        iterate = symmetric * (jnp.sqrt(live_order) / (2.0 * jnp.sqrt(total + 1e-06)))
        parts = split(iterate)
        square = split(product(jnp.concatenate(parts, axis=0), parts))

        def times_square(value):
            return product(stack(value), square)

        home = iterate[:BLK]
        home = 1.5 * home - 0.5 * times_square(home)
        cube = times_square(home)
        cube = 1.5 * cube - 0.5 * times_square(cube)
        cube = 1.5 * cube - 0.5 * times_square(cube)
        home = 1.5 * home - 0.5 * cube
        diagonal = lax.broadcasted_iota(jnp.int32, (BLK, order), 0) == lax.broadcasted_iota(
            jnp.int32, (BLK, order), 1
        )
        home = 0.5 * (jnp.where(diagonal, 1.0, 0.0) - home)
        tiles = [jnp.zeros((BLK, chunk), F32) for _ in range(window // chunk)]
        for p in range(maxb):
            other = pos_ref[g, p]
            sub = lax.rem(other, groups)
            t = p // groups
            value = home[:, t * chunk : (t + 1) * chunk]
            value = turn(value, lax.rem(sub + groups - p % groups, groups))
            value = jnp.where(lane_group == jnp.full((BLK, chunk), sub, jnp.int32), value, 0.0)
            place = jnp.full((BLK, chunk), lax.div(other, groups), jnp.int32)
            value = jnp.where(jnp.full((BLK, chunk), live, jnp.int32) > p, value, 0.0)
            for m in range(len(tiles)):
                tiles[m] += jnp.where(place == m, value, 0.0)
        for m, tile in enumerate(tiles):
            band_v[g, :, m * chunk : (m + 1) * chunk] = tile
        return carry

    lax.fori_loop(0, own_blocks, solve, 0)

    stacked = stack(band_v[...].reshape(own, window))
    for b in range(3):
        total = None
        for a in (0, 1, 2):
            if abs(a - b) > 1:
                continue
            term = product(stacked[:, a * slab : (a + 1) * slab], (wide_hi[a, b], wide_lo[a, b]))
            total = term if total is None else total + term
        rows_v[b] = mask_b[:, b * slab : (b + 1) * slab] * total

    def lanes_of(k):
        return pl.ds(pl.multiple_of(chunk * k, chunk), chunk)

    back = []
    for offset in (2, 1, 3, 0):
        target = lax.rem(col + offset, cols)
        origin = lax.rem(col + cols - offset, cols)
        for a, span, device in ((0, (1, 2), above), (2, (0, 2), below)):
            copy = send(
                rows_v.at[pl.ds(*span), :, lanes_of(target)],
                back_v.at[a, pl.ds(*spans[a]), col, space],
                {"rows": device, "cols": target},
            )
            back.append((a, origin, copy))
    for offset in (2, 1, 3):
        target = lax.rem(col + offset, cols)
        origin = lax.rem(col + cols - offset, cols)
        copy = send(
            rows_v.at[:, :, lanes_of(target)],
            back_v.at[1, :, col, space],
            {"cols": target},
        )
        back.append((1, origin, copy))
    back_mate = [send(rows_v.at[:, :, lanes], back_v.at[1, :, col, space], mate)]
    back_v[1, :, col, space] = rows_v[:, :, lanes]
    for a, origin, copy in sorted(back, key=lambda item: item[0] != 1):
        copy.wait_recv()
        piece = back_v.at[a, pl.ds(*spans[a]), origin, space]
        back_mate.append(send(piece, piece, mate))
        if len(back_mate) == cols:
            for other in back_mate:
                other.wait_recv()
            acc_v[...] = product(left_block(1), window_block(back_v, 1))
    for other in back_mate[cols:]:
        other.wait_recv()
    done = combine(
        product(left_block(0), window_block(back_v, 0)),
        acc_v[...],
        product(left_block(2), window_block(back_v, 2)),
        chunk,
    )
    for b in range(3):
        masked = mask_a[:, :, b * chunk : (b + 1) * chunk].reshape(half, chunk)
        piece = masked * done[:, b * chunk : (b + 1) * chunk]
        strip_v[:, b] = piece.reshape(cols, own, chunk)
    outs = []
    for offset in (2, 1, 3):
        target = lax.rem(col + offset, cols)
        outs.append(send(strip_v.at[target], final_v.at[col], {"cols": target}))
    final_v[col] = strip_v[col]
    for copy in outs:
        copy.wait_recv()
    total = jnp.zeros((own, chunk), F32)
    for b in range(3):
        for k in range(cols):
            value = final_v[k, b]
            total = total + value
            density_ref[:, b * slab + k * chunk : b * slab + (k + 1) * chunk] = value
    charges_ref[...] = jnp.sum(total.T, axis=0, keepdims=True)
    send.finish()


def shards(hamiltonian, correlation_root, pattern, sub_blocks, sub_count):
    slab, window = correlation_root.shape
    own = hamiltonian.shape[0]
    cols = lax.axis_size("cols")
    chunk = slab // cols
    half = slab // 2
    own_blocks, maxb = sub_blocks.shape
    order = maxb * BLK
    vmem = functools.partial(pltpu.VMEM)
    density, charges = pl.pallas_call(
        kernel,
        out_shape=[
            jax.ShapeDtypeStruct((own, window), F32),
            jax.ShapeDtypeStruct((1, own), F32),
        ],
        in_specs=[
            pl.BlockSpec(memory_space=pltpu.SMEM),
            pl.BlockSpec(memory_space=pltpu.SMEM),
            pl.BlockSpec(memory_space=pl.ANY),
            pl.BlockSpec(memory_space=pl.ANY),
            pl.BlockSpec(memory_space=pltpu.VMEM),
        ],
        out_specs=[pl.BlockSpec(memory_space=pltpu.VMEM)] * 2,
        scratch_shapes=[
            vmem((slab, window), F32),
            vmem((2, half, window), BF16),
            vmem((cols, own, window), F32),
            vmem((2, 2, slab, slab), F32),
            vmem((3, 3, slab, slab), BF16),
            vmem((3, 3, slab, slab), BF16),
            vmem((3, slab, 3 * chunk), BF16),
            vmem((3, slab, 3 * chunk), BF16),
            vmem((cols, own, 3 * chunk), F32),
            vmem((own, window), F32),
            vmem((3, 3, cols, 2, own, chunk), F32),
            vmem((3, 3, cols, 2, own, chunk), F32),
            vmem((3, 3, 2, half // BLK, cols, BLK, chunk), F32),
            vmem((half, 3 * chunk), F32),
            vmem((order, order), F32),
            vmem((own_blocks, BLK, window), F32),
            vmem((3, own, slab), F32),
            vmem((cols, 3, own, chunk), F32),
            vmem((cols, 3, own, chunk), F32),
            pltpu.SemaphoreType.DMA((2,)),
            pltpu.SemaphoreType.DMA((160,)),
            pltpu.SemaphoreType.DMA((160,)),
        ],
        compiler_params=pltpu.CompilerParams(
            collective_id=1, has_side_effects=True, vmem_limit_bytes=60 * 2**20
        ),
    )(sub_blocks, sub_count, hamiltonian, correlation_root, pattern)
    return density, charges.reshape(own)


def solution(mesh):
    return jax.shard_map(
        shards,
        mesh=mesh,
        in_specs=(
            P(("rows", "cols", "space"), None),
            P("rows", None),
            P(),
            P(("rows", "cols", "space"), None),
            P(("rows", "cols", "space")),
        ),
        out_specs=(P(("rows", "cols", "space"), None), P(("rows", "cols", "space"))),
        check_vma=False,
    )
```

```python
import functools

import jax
import jax.numpy as jnp
from jax import lax
from jax.experimental import pallas as pl
from jax.experimental.pallas import tpu as pltpu
from jax.sharding import PartitionSpec as P

BLK = 32
F32 = jnp.float32
BF16 = jnp.bfloat16


def split(value):
    upper = value.astype(BF16)
    return upper, (value - upper.astype(F32)).astype(BF16)


def dot(leftside, rightside):
    return jnp.dot(leftside, rightside, preferred_element_type=F32)


def product(stacked, right):
    high, low = right
    half = stacked.shape[0] // 2
    both = dot(stacked, high)
    return both[:half] + both[half:] + dot(stacked[:half], low)


def stack(value):
    return jnp.concatenate(split(value), axis=0)


def combine(above, own, below, width):
    return jnp.concatenate(
        [
            above[:, :width] + own[:, :width],
            above[:, width:] + own[:, width : 2 * width] + below[:, :width],
            own[:, 2 * width :] + below[:, width:],
        ],
        axis=1,
    )


class Sender:
    def __init__(self, send_sems, recv_sems):
        self.sems = (send_sems, recv_sems)
        self.copies = []

    def __call__(self, source, target, device):
        slot = len(self.copies)
        copy = pltpu.make_async_remote_copy(
            src_ref=source,
            dst_ref=target,
            send_sem=self.sems[0].at[slot],
            recv_sem=self.sems[1].at[slot],
            device_id=device,
            device_id_type=pl.DeviceIdType.MESH,
        )
        copy.start()
        self.copies.append(copy)
        return copy

    def finish(self):
        for copy in self.copies:
            copy.wait_send()


def kernel(
    pos_ref,
    count_ref,
    ham_ref,
    root_ref,
    pattern_ref,
    density_ref,
    charges_ref,
    root_v,
    left_s,
    ham_v,
    land_v,
    wide_hi,
    wide_lo,
    near_hi,
    near_lo,
    mask_a,
    mask_b,
    half_v,
    back_v,
    ortho_v,
    acc_v,
    sub_v,
    turns_v,
    rows_v,
    strip_v,
    final_v,
    local_sems,
    send_sems,
    recv_sems,
):
    row = lax.axis_index("rows")
    count = lax.axis_size("rows")
    col = lax.axis_index("cols")
    space = lax.axis_index("space")
    cols = lax.axis_size("cols")
    slab, window = root_v.shape
    own = ham_ref.shape[0]
    chunk = slab // cols
    half = slab // 2
    maxb = pos_ref.shape[1]
    slab_blocks = slab // BLK
    own_blocks = own // BLK
    order = maxb * BLK
    groups = chunk // BLK

    first = col + 1 - 2 * lax.rem(col, 2)
    second = lax.rem(col + 2, 4)
    third = lax.rem(first + 2, 4)
    above = lax.rem(row + 1, count)
    below = lax.rem(row + count - 1, count)
    up, down = {"rows": above}, {"rows": below}
    side, cross, mate = {"cols": first}, {"cols": second}, {"space": 1 - space}
    lanes = pl.ds(pl.multiple_of(chunk * col, chunk), chunk)

    load_root = pltpu.make_async_copy(root_ref, root_v, local_sems.at[0])
    load_ham = pltpu.make_async_copy(ham_ref, ham_v.at[col], local_sems.at[1])
    load_root.start()
    load_ham.start()

    barrier = pltpu.get_barrier_semaphore()
    peers = [mate]
    for offset in range(cols):
        other = lax.rem(col + offset, cols)
        peers += [{"rows": above, "cols": other}, {"rows": below, "cols": other}]
        if offset:
            peers.append({"cols": other})
    for peer in peers:
        pl.semaphore_signal(barrier, inc=1, device_id=peer, device_id_type=pl.DeviceIdType.MESH)
    pl.semaphore_wait(barrier, len(peers))
    send = Sender(send_sems, recv_sems)

    ham_first = send(ham_ref, ham_v.at[col], side)
    ham_second = send(ham_ref, ham_v.at[col], cross)

    def land(piece, k, part=None):
        size = half if part is None else half // 2
        start = half * space + (0 if part is None else part * size)
        return land_v.at[
            piece // 2,
            piece % 2,
            pl.ds(pl.multiple_of(start, size), size),
            pl.ds(pl.multiple_of(chunk * k, chunk), chunk),
        ]

    order_of_pieces = (0, 2, 1, 3)
    pieces = {}
    for piece in order_of_pieces:
        panel = (1, 2, 1, 0)[piece]
        source = root_ref.at[
            pl.ds(pl.multiple_of(half * space, half), half),
            pl.ds(pl.multiple_of(panel * slab + chunk * col, chunk), chunk),
        ]
        pieces[piece] = send(source, land(piece, col), up if piece < 2 else down)

    zero = jnp.zeros(ortho_v.shape[3:], F32)
    for part in range(2):
        ortho_v[0, 2, part] = zero
        ortho_v[2, 0, part] = zero

    pattern = pattern_ref[...].astype(F32).astype(BF16)
    blocks_all = pattern.shape[1]

    def pick(rows, block_of):
        wanted = block_of(lax.broadcasted_iota(jnp.int32, (rows, blocks_all), 0))
        here = lax.broadcasted_iota(jnp.int32, (rows, blocks_all), 1)
        chosen = jnp.where(wanted == here, 1.0, 0.0).astype(BF16)
        return lax.dot_general(
            chosen, pattern, (((1,), (1,)), ((), ())), preferred_element_type=F32
        ).astype(BF16)

    def spread(values, wanted):
        here = lax.broadcasted_iota(jnp.int32, wanted.shape, 0)
        return dot(values, jnp.where(wanted == here, 1.0, 0.0).astype(BF16))

    base = row * slab_blocks
    strip_rows = pick(
        cols * own,
        lambda i: base + ((i // own) * 2 + space) * own_blocks + (i % own) // BLK,
    )
    lane = lax.broadcasted_iota(jnp.int32, (3 * slab_blocks, 3 * chunk), 1)
    chip_mask = spread(
        strip_rows, (lane // chunk) * slab_blocks + col * groups + (lane % chunk) // BLK
    )
    for i in range(cols):
        mask_a[i] = chip_mask[i * own : (i + 1) * own]
    own_rows = pick(own, lambda i: base + (col * 2 + space) * own_blocks + i // BLK)
    lane = lax.broadcasted_iota(jnp.int32, (3 * slab_blocks, window), 1)
    mask_b[...] = spread(own_rows, lane // BLK)

    load_root.wait()
    for i in range(cols):
        start = pl.multiple_of((i * 2 + space) * own, own)
        upper, lower = split(root_v[pl.ds(start, own), :])
        left_s[0, i * own : (i + 1) * own] = upper
        left_s[1, i * own : (i + 1) * own] = lower
    for b in range(3):
        wide_hi[1, b], wide_lo[1, b] = split(root_v[:, b * slab : (b + 1) * slab])
        start = pl.multiple_of(b * slab + chunk * col, chunk)
        upper, lower = split(root_v[:, pl.ds(start, chunk)])
        near_hi[1, :, b * chunk : (b + 1) * chunk] = upper
        near_lo[1, :, b * chunk : (b + 1) * chunk] = lower

    relayed = {}
    gathers = {}

    def arrive(piece):
        pieces[piece].wait_recv()
        relayed[piece] = send(land(piece, col), land(piece, col), mate)

    def offer(piece):
        gathers[piece] = [
            send(land(piece, col), land(piece, col), side),
            send(land(piece, col), land(piece, col), cross),
        ]

    def half_rows(k, part):
        return ham_v.at[k, pl.ds(part * (own // 2), own // 2), :]

    arrive(0)
    arrive(2)
    ham_first.wait_recv()
    ham_half_a = send(half_rows(first, 1), half_rows(first, 1), cross)
    ham_second.wait_recv()
    ham_half_b = send(half_rows(second, 0), half_rows(second, 0), side)
    offer(0)
    offer(2)
    arrive(1)
    arrive(3)
    offer(1)
    offer(3)
    for piece in order_of_pieces:
        relayed[piece].wait_recv()
        upper, lower = split(land_v[piece // 2, piece % 2, :, lanes])
        side_of = 0 if piece < 2 else 2
        place = (0, 1, 1, 0)[piece]
        near_hi[side_of, :, place * chunk : (place + 1) * chunk] = upper
        near_lo[side_of, :, place * chunk : (place + 1) * chunk] = lower

    load_ham.wait()
    strips = (col, first, second, third)
    half_up, half_down, half_mate = [], [], []
    for i, strip in enumerate(strips):
        if i == 3:
            ham_half_a.wait_recv()
            ham_half_b.wait_recv()
        stacked = stack(ham_v[strip])
        terms = []
        for a in range(3):
            width = 3 * chunk if a == 1 else 2 * chunk
            terms.append(
                product(
                    stacked[:, a * slab : (a + 1) * slab],
                    (near_hi[a, :, :width], near_lo[a, :, :width]),
                )
            )
        done = mask_a[strip] * combine(*terms, chunk)
        for b in range(3):
            half_v[1, b, strip, space] = done[:, b * chunk : (b + 1) * chunk]
        half_up.append(
            send(
                half_v.at[1, pl.ds(1, 2), strip, space],
                half_v.at[0, pl.ds(0, 2), strip, space],
                up,
            )
        )
        half_down.append(
            send(
                half_v.at[1, pl.ds(0, 2), strip, space],
                half_v.at[2, pl.ds(1, 2), strip, space],
                down,
            )
        )
        half_mate.append(
            send(half_v.at[1, :, strip, space], half_v.at[1, :, strip, space], mate)
        )

    def window_block(ref, a):
        picked = {0: (0, 1), 1: (0, 1, 2), 2: (1, 2)}[a]
        return split(
            jnp.concatenate([ref[a, b].reshape(slab, chunk) for b in picked], axis=1)
        )

    def left_block(a):
        return left_s[:, :, a * slab : (a + 1) * slab].reshape(2 * half, slab)

    for copy in half_mate:
        copy.wait_recv()
    acc_v[...] = product(left_block(1), window_block(half_v, 1))
    relays = []
    mates = []
    for i, piece in enumerate(order_of_pieces):
        gathers[piece][0].wait_recv()
        relays.append(send(land(piece, first, 1), land(piece, first, 1), cross))
        mates.append(send(land(piece, first), land(piece, first), mate))
        gathers[piece][1].wait_recv()
        relays.append(send(land(piece, second, 0), land(piece, second, 0), side))
        mates.append(send(land(piece, second), land(piece, second), mate))
        half_up[i].wait_recv()
        region = half_v.at[0, pl.ds(0, 2), strips[i], space]
        half_mate.append(send(region, region, mate))
        half_down[i].wait_recv()
        region = half_v.at[2, pl.ds(1, 2), strips[i], space]
        half_mate.append(send(region, region, mate))
    for copy in half_mate[cols:]:
        copy.wait_recv()

    done = combine(
        product(left_block(0), window_block(half_v, 0)),
        acc_v[...],
        product(left_block(2), window_block(half_v, 2)),
        chunk,
    )
    for b in range(3):
        masked = mask_a[:, :, b * chunk : (b + 1) * chunk].reshape(half, chunk)
        masked = masked * done[:, b * chunk : (b + 1) * chunk]
        ortho_v[1, b, space, :, col] = masked.reshape(half // BLK, BLK, chunk)

    spans = {0: (0, 2), 1: (0, 3), 2: (1, 2)}

    def region(a, k, part=None, span=None):
        size = half // BLK if part is None else half // BLK // 2
        start = 0 if part is None else part * size
        return ortho_v.at[a, pl.ds(*(span or spans[a])), space, pl.ds(start, size), k]

    def pass_on(a, k, part, device):
        return send(region(a, k, part), region(a, k, part), device)

    def to_rows(k, part):
        return (
            send(region(1, k, part, (1, 2)), region(0, k, part), up),
            send(region(1, k, part, (0, 2)), region(2, k, part), down),
        )

    pending = []
    own_rows_out = to_rows(col, None)
    own_first = pass_on(1, col, None, side)
    own_second = pass_on(1, col, None, cross)
    pending.append(pass_on(1, col, None, mate))
    for copy in relays:
        copy.wait_recv()
    for piece in order_of_pieces:
        mates.append(send(land(piece, third), land(piece, third), mate))
    for copy in mates:
        copy.wait_recv()
    for piece in order_of_pieces:
        a = 0 if piece < 2 else 2
        b = (0, 1, 2, 1)[piece]
        wide_hi[a, b], wide_lo[a, b] = split(land_v[piece // 2, piece % 2])

    own_first.wait_recv()
    diagonal_a = pass_on(1, first, 1, cross)
    first_rows = to_rows(first, 0)
    pending.append(pass_on(1, first, None, mate))
    own_second.wait_recv()
    diagonal_b = pass_on(1, second, 0, side)
    second_rows = to_rows(second, 1)
    pending.append(pass_on(1, second, None, mate))
    hops = []
    for a, copy in ((0, own_rows_out[0]), (2, own_rows_out[1])):
        copy.wait_recv()
        hops.append((a, first, 1, pass_on(a, col, 1, side)))
        hops.append((a, second, 0, pass_on(a, col, 0, cross)))
        pending.append(pass_on(a, col, None, mate))
    diagonal_a.wait_recv()
    diagonal_b.wait_recv()
    pending.append(pass_on(1, third, None, mate))
    for a, copy in ((0, first_rows[0]), (2, first_rows[1])):
        copy.wait_recv()
        hops.append((a, third, 0, pass_on(a, first, 0, cross)))
        pending.append(pass_on(a, first, 0, mate))
    for a, copy in ((0, second_rows[0]), (2, second_rows[1])):
        copy.wait_recv()
        hops.append((a, third, 1, pass_on(a, second, 1, side)))
        pending.append(pass_on(a, second, 1, mate))
    for a, k, part, copy in hops:
        copy.wait_recv()
        pending.append(pass_on(a, k, part, mate))
    for copy in pending:
        copy.wait_recv()

    lane_group = lax.broadcasted_iota(jnp.int32, (8, chunk), 1) // BLK

    def solve(g):
        live = count_ref[g]

        for p in range(maxb):
            sub = lax.rem(pos_ref[g, p], groups)
            steps = lax.rem(p + groups - sub, groups)
            turns_v[p] = jnp.where(
                lane_group == jnp.full(lane_group.shape, sub, jnp.int32),
                jnp.full(lane_group.shape, steps, jnp.int32),
                -1,
            )

        def assemble(i, inner):
            block = pos_ref[g, i]
            a = lax.div(block, slab_blocks)
            within = lax.rem(block, slab_blocks)
            owner = lax.div(within, own_blocks)
            core = lax.rem(owner, 2)
            place = lax.div(owner, 2) * own_blocks + lax.rem(within, own_blocks)
            for t in range(maxb // groups):
                sorted_by = [jnp.zeros((BLK, chunk), F32)] * groups
                for e in range(groups):
                    p = t * groups + e
                    other = pos_ref[g, p]
                    b = lax.div(other, slab_blocks)
                    k = lax.div(lax.rem(other, slab_blocks), groups)
                    value = ortho_v[a, b, core, place, k]
                    needed = jnp.tile(turns_v[p], (BLK // 8, 1))
                    for steps in range(groups):
                        sorted_by[steps] = jnp.where(needed == steps, value, sorted_by[steps])
                tile = sorted_by[0]
                for steps in range(1, groups):
                    tile = tile + pltpu.roll(sorted_by[steps], steps * BLK, 1)
                sub_v[pl.ds(pl.multiple_of(i * BLK, BLK), BLK), t * chunk : (t + 1) * chunk] = tile
            return inner

        lax.fori_loop(0, maxb, assemble, 0)
        position = [lax.broadcasted_iota(jnp.int32, (order, order), d) for d in range(2)]
        assembled = jnp.where(jnp.maximum(*position) < live * BLK, sub_v[...], 0.0)
        symmetric = 0.5 * (assembled + assembled.T)
        total = jnp.sum(jnp.sum(symmetric * symmetric, axis=1, keepdims=True), axis=0, keepdims=True)
        live_order = jnp.full((1, 1), live * BLK, jnp.int32).astype(F32)
        iterate = symmetric * (jnp.sqrt(live_order) / (2.0 * jnp.sqrt(total + 1e-06)))
        parts = split(iterate)
        square = split(dot(parts[0], parts[0]) + dot(parts[0], parts[1]) + dot(parts[1], parts[0]))

        def times_square(value):
            return product(stack(value), square)

        home = iterate[:BLK]
        home = 1.5 * home - 0.5 * times_square(home)
        cube = times_square(home)
        cube = 1.5 * cube - 0.5 * times_square(cube)
        cube = 1.5 * cube - 0.5 * times_square(cube)
        home = 1.5 * home - 0.5 * cube
        diagonal = lax.broadcasted_iota(jnp.int32, (BLK, order), 0) == lax.broadcasted_iota(
            jnp.int32, (BLK, order), 1
        )
        home = 0.5 * (jnp.where(diagonal, 1.0, 0.0) - home)
        tiles = [jnp.zeros((BLK, chunk), F32) for _ in range(window // chunk)]
        turned = [
            [home[:, t * chunk : (t + 1) * chunk]]
            + [
                pltpu.roll(home[:, t * chunk : (t + 1) * chunk], steps * BLK, 1)
                for steps in range(1, groups)
            ]
            for t in range(maxb // groups)
        ]
        for p in range(maxb):
            other = pos_ref[g, p]
            sub = lax.rem(other, groups)
            here = (lane_group == jnp.full(lane_group.shape, sub, jnp.int32)) & (
                jnp.full(lane_group.shape, live, jnp.int32) > p
            )
            place = jnp.where(
                here, jnp.full(lane_group.shape, lax.div(other, groups), jnp.int32), -1
            )
            place = jnp.tile(place, (BLK // 8, 1))
            ways = turned[p // groups]
            wide = jnp.tile(lane_group, (BLK // 8, 1))
            value = ways[(groups - p) % groups]
            for target in range(1, groups):
                value = jnp.where(wide == target, ways[(target + groups - p) % groups], value)
            for m in range(len(tiles)):
                tiles[m] = jnp.where(place == m, value, tiles[m])
        return jnp.concatenate(tiles, axis=1)

    def lanes_of(k):
        return pl.ds(pl.multiple_of(chunk * k, chunk), chunk)

    back, back_mate = [], []
    for g in range(own_blocks):
        stacked = stack(solve(g))
        these = slice(g * BLK, (g + 1) * BLK)
        for b in range(3):
            total = None
            for a in (0, 1, 2):
                if abs(a - b) > 1:
                    continue
                term = product(
                    stacked[:, a * slab : (a + 1) * slab], (wide_hi[a, b], wide_lo[a, b])
                )
                total = term if total is None else total + term
            rows_v[b, these] = mask_b[these, b * slab : (b + 1) * slab] * total
        these = pl.ds(g * BLK, BLK)
        for offset in (2, 1, 3, 0):
            target = lax.rem(col + offset, cols)
            origin = lax.rem(col + cols - offset, cols)
            for a, span, device in ((0, (1, 2), above), (2, (0, 2), below)):
                copy = send(
                    rows_v.at[pl.ds(*span), these, lanes_of(target)],
                    back_v.at[a, pl.ds(*spans[a]), col, space, these],
                    {"rows": device, "cols": target},
                )
                back.append((a, g, origin, copy))
        for offset in (2, 1, 3):
            target = lax.rem(col + offset, cols)
            origin = lax.rem(col + cols - offset, cols)
            copy = send(
                rows_v.at[:, these, lanes_of(target)],
                back_v.at[1, :, col, space, these],
                {"cols": target},
            )
            back.append((1, g, origin, copy))
        back_mate.append(
            send(rows_v.at[:, these, lanes], back_v.at[1, :, col, space, these], mate)
        )
    back_v[1, :, col, space] = rows_v[:, :, lanes]
    for a, g, origin, copy in sorted(back, key=lambda item: (item[0] != 1, item[1])):
        copy.wait_recv()
        piece = back_v.at[a, pl.ds(*spans[a]), origin, space, pl.ds(g * BLK, BLK)]
        back_mate.append(send(piece, piece, mate))
        if len(back_mate) == own_blocks * cols:
            for other in back_mate:
                other.wait_recv()
            acc_v[...] = product(left_block(1), window_block(back_v, 1))
    for other in back_mate[own_blocks * cols :]:
        other.wait_recv()
    done = combine(
        product(left_block(0), window_block(back_v, 0)),
        acc_v[...],
        product(left_block(2), window_block(back_v, 2)),
        chunk,
    )
    for b in range(3):
        masked = mask_a[:, :, b * chunk : (b + 1) * chunk].reshape(half, chunk)
        piece = masked * done[:, b * chunk : (b + 1) * chunk]
        strip_v[:, b] = piece.reshape(cols, own, chunk)
    outs = []
    for offset in (2, 1, 3):
        target = lax.rem(col + offset, cols)
        outs.append(send(strip_v.at[target], final_v.at[col], {"cols": target}))
    final_v[col] = strip_v[col]
    for copy in outs:
        copy.wait_recv()
    total = jnp.zeros((own, chunk), F32)
    for b in range(3):
        for k in range(cols):
            value = final_v[k, b]
            total = total + value
            density_ref[:, b * slab + k * chunk : b * slab + (k + 1) * chunk] = value
    charges_ref[...] = jnp.sum(total.T, axis=0)
    send.finish()


def place_kernel(density_ref, charges_ref, density_out, charges_out, density_v, charges_v, sems):
    inward = [
        pltpu.make_async_copy(density_ref, density_v, sems.at[0]),
        pltpu.make_async_copy(charges_ref, charges_v, sems.at[1]),
    ]
    outward = [
        pltpu.make_async_copy(density_v, density_out, sems.at[2]),
        pltpu.make_async_copy(charges_v, charges_out, sems.at[3]),
    ]
    for copy in inward:
        copy.start()
    for copy, then in zip(inward, outward):
        copy.wait()
        then.start()
    for copy in outward:
        copy.wait()


def shards(hamiltonian, correlation_root, pattern, sub_blocks, sub_count):
    slab, window = correlation_root.shape
    own = hamiltonian.shape[0]
    cols = lax.axis_size("cols")
    chunk = slab // cols
    half = slab // 2
    own_blocks, maxb = sub_blocks.shape
    order = maxb * BLK
    vmem = functools.partial(pltpu.VMEM)
    density, charges = pl.pallas_call(
        kernel,
        out_shape=[
            jax.ShapeDtypeStruct((own, window), F32),
            jax.ShapeDtypeStruct((own,), F32),
        ],
        in_specs=[
            pl.BlockSpec(memory_space=pltpu.SMEM),
            pl.BlockSpec(memory_space=pltpu.SMEM),
            pl.BlockSpec(memory_space=pltpu.HBM),
            pl.BlockSpec(memory_space=pltpu.HBM),
            pl.BlockSpec(memory_space=pltpu.VMEM),
        ],
        out_specs=[pl.BlockSpec(memory_space=pltpu.VMEM)] * 2,
        scratch_shapes=[
            vmem((slab, window), F32),
            vmem((2, half, window), BF16),
            vmem((cols, own, window), F32),
            vmem((2, 2, slab, slab), F32),
            vmem((3, 3, slab, slab), BF16),
            vmem((3, 3, slab, slab), BF16),
            vmem((3, slab, 3 * chunk), BF16),
            vmem((3, slab, 3 * chunk), BF16),
            vmem((cols, own, 3 * chunk), F32),
            vmem((own, window), F32),
            vmem((3, 3, cols, 2, own, chunk), F32),
            vmem((3, 3, cols, 2, own, chunk), F32),
            vmem((3, 3, 2, half // BLK, cols, BLK, chunk), F32),
            vmem((half, 3 * chunk), F32),
            vmem((order, order), F32),
            vmem((maxb, 8, chunk), jnp.int32),
            vmem((3, own, slab), F32),
            vmem((cols, 3, own, chunk), F32),
            vmem((cols, 3, own, chunk), F32),
            pltpu.SemaphoreType.DMA((2,)),
            pltpu.SemaphoreType.DMA((200,)),
            pltpu.SemaphoreType.DMA((200,)),
        ],
        compiler_params=pltpu.CompilerParams(
            collective_id=1, has_side_effects=True, vmem_limit_bytes=62 * 2**20
        ),
    )(sub_blocks, sub_count, hamiltonian, correlation_root, pattern.T)
    return pl.pallas_call(
        place_kernel,
        out_shape=[
            jax.ShapeDtypeStruct((own, window), F32),
            jax.ShapeDtypeStruct((own,), F32),
        ],
        in_specs=[pl.BlockSpec(memory_space=pltpu.HBM)] * 2,
        out_specs=[pl.BlockSpec(memory_space=pltpu.HBM)] * 2,
        scratch_shapes=[
            pltpu.VMEM((own, window), F32),
            pltpu.VMEM((own,), F32),
            pltpu.SemaphoreType.DMA((4,)),
        ],
        compiler_params=pltpu.CompilerParams(vmem_limit_bytes=62 * 2**20),
    )(density, charges)


def solution(mesh):
    return jax.shard_map(
        shards,
        mesh=mesh,
        in_specs=(
            P(("rows", "cols", "space"), None),
            P("rows", None),
            P(),
            P(("rows", "cols", "space"), None),
            P(("rows", "cols", "space")),
        ),
        out_specs=(P(("rows", "cols", "space"), None), P(("rows", "cols", "space"))),
        check_vma=False,
    )
```

```python
import functools

import jax
import jax.numpy as jnp
from jax import lax
from jax.experimental import pallas as pl
from jax.experimental.pallas import tpu as pltpu
from jax.sharding import PartitionSpec as P

BLK = 32
F32 = jnp.float32
BF16 = jnp.bfloat16


def split(value):
    upper = value.astype(BF16)
    return upper, (value - upper.astype(F32)).astype(BF16)


def dot(leftside, rightside):
    return jnp.dot(leftside, rightside, preferred_element_type=F32)


def product(stacked, right):
    high, low = right
    half = stacked.shape[0] // 2
    both = dot(stacked, high)
    return both[:half] + both[half:] + dot(stacked[:half], low)


def stack(value):
    return jnp.concatenate(split(value), axis=0)


def combine(above, own, below, width):
    return jnp.concatenate(
        [
            above[:, :width] + own[:, :width],
            above[:, width:] + own[:, width : 2 * width] + below[:, :width],
            own[:, 2 * width :] + below[:, width:],
        ],
        axis=1,
    )


class Sender:
    def __init__(self, send_sems, recv_sems):
        self.sems = (send_sems, recv_sems)
        self.copies = []

    def __call__(self, source, target, device):
        slot = len(self.copies)
        copy = pltpu.make_async_remote_copy(
            src_ref=source,
            dst_ref=target,
            send_sem=self.sems[0].at[slot],
            recv_sem=self.sems[1].at[slot],
            device_id=device,
            device_id_type=pl.DeviceIdType.MESH,
        )
        copy.start()
        self.copies.append(copy)
        return copy

    def finish(self):
        for copy in self.copies:
            copy.wait_send()


def kernel(
    pos_in,
    count_in,
    ham_ref,
    root_ref,
    pattern_in,
    density_ref,
    charges_ref,
    root_v,
    left_s,
    ham_v,
    land_v,
    wide_hi,
    wide_lo,
    near_hi,
    near_lo,
    mask_a,
    mask_b,
    half_v,
    back_v,
    ortho_v,
    acc_v,
    sub_v,
    turns_v,
    rows_v,
    strip_v,
    final_v,
    pattern_ref,
    pos_ref,
    count_ref,
    table_s,
    local_sems,
    send_sems,
    recv_sems,
):
    row = lax.axis_index("rows")
    count = lax.axis_size("rows")
    col = lax.axis_index("cols")
    space = lax.axis_index("space")
    cols = lax.axis_size("cols")
    slab, window = root_v.shape
    own = ham_ref.shape[0]
    chunk = slab // cols
    half = slab // 2
    maxb = pos_ref.shape[1]
    slab_blocks = slab // BLK
    own_blocks = own // BLK
    order = maxb * BLK
    groups = chunk // BLK

    first = col + 1 - 2 * lax.rem(col, 2)
    second = lax.rem(col + 2, 4)
    third = lax.rem(first + 2, 4)
    above = lax.rem(row + 1, count)
    below = lax.rem(row + count - 1, count)
    up, down = {"rows": above}, {"rows": below}
    side, cross, mate = {"cols": first}, {"cols": second}, {"space": 1 - space}
    lanes = pl.ds(pl.multiple_of(chunk * col, chunk), chunk)

    load_root = pltpu.make_async_copy(root_ref, root_v, local_sems.at[0])
    load_ham = pltpu.make_async_copy(ham_ref, ham_v.at[col], local_sems.at[1])
    small = [
        pltpu.make_async_copy(pos_in, pos_ref, local_sems.at[2]),
        pltpu.make_async_copy(count_in, count_ref, local_sems.at[3]),
        pltpu.make_async_copy(pattern_in, pattern_ref, local_sems.at[4]),
    ]
    load_root.start()
    load_ham.start()
    for copy in small:
        copy.start()

    barrier = pltpu.get_barrier_semaphore()
    peers = [mate]
    for offset in range(cols):
        other = lax.rem(col + offset, cols)
        peers += [{"rows": above, "cols": other}, {"rows": below, "cols": other}]
        if offset:
            peers.append({"cols": other})
    for peer in peers:
        pl.semaphore_signal(barrier, inc=1, device_id=peer, device_id_type=pl.DeviceIdType.MESH)
    pl.semaphore_wait(barrier, len(peers))
    send = Sender(send_sems, recv_sems)

    ham_first = send(ham_ref, ham_v.at[col], side)
    ham_second = send(ham_ref, ham_v.at[col], cross)

    def land(piece, k, part=None):
        size = half if part is None else half // 2
        start = half * space + (0 if part is None else part * size)
        return land_v.at[
            piece // 2,
            piece % 2,
            pl.ds(pl.multiple_of(start, size), size),
            pl.ds(pl.multiple_of(chunk * k, chunk), chunk),
        ]

    order_of_pieces = (0, 2, 1, 3)
    pieces = {}
    for piece in order_of_pieces:
        panel = (1, 2, 1, 0)[piece]
        source = root_ref.at[
            pl.ds(pl.multiple_of(half * space, half), half),
            pl.ds(pl.multiple_of(panel * slab + chunk * col, chunk), chunk),
        ]
        pieces[piece] = send(source, land(piece, col), up if piece < 2 else down)

    zero = jnp.zeros(ortho_v.shape[3:], F32)
    for part in range(2):
        ortho_v[0, 2, part] = zero
        ortho_v[2, 0, part] = zero

    for copy in small:
        copy.wait()
    pattern = pattern_ref[...].astype(F32).astype(BF16)
    blocks_all = pattern.shape[1]

    def pick(rows, block_of):
        wanted = block_of(lax.broadcasted_iota(jnp.int32, (rows, blocks_all), 0))
        here = lax.broadcasted_iota(jnp.int32, (rows, blocks_all), 1)
        chosen = jnp.where(wanted == here, 1.0, 0.0).astype(BF16)
        return lax.dot_general(
            chosen, pattern, (((1,), (1,)), ((), ())), preferred_element_type=F32
        ).astype(BF16)

    def spread(values, wanted):
        here = lax.broadcasted_iota(jnp.int32, wanted.shape, 0)
        return dot(values, jnp.where(wanted == here, 1.0, 0.0).astype(BF16))

    base = row * slab_blocks
    strip_rows = pick(
        cols * own,
        lambda i: base + ((i // own) * 2 + space) * own_blocks + (i % own) // BLK,
    )
    lane = lax.broadcasted_iota(jnp.int32, (3 * slab_blocks, 3 * chunk), 1)
    chip_mask = spread(
        strip_rows, (lane // chunk) * slab_blocks + col * groups + (lane % chunk) // BLK
    )
    for i in range(cols):
        mask_a[i] = chip_mask[i * own : (i + 1) * own]
    own_rows = pick(own, lambda i: base + (col * 2 + space) * own_blocks + i // BLK)
    lane = lax.broadcasted_iota(jnp.int32, (3 * slab_blocks, window), 1)
    mask_b[...] = spread(own_rows, lane // BLK)

    for g in range(own_blocks):
        for p in range(maxb):
            block = pos_ref[g, p]
            within = lax.rem(block, slab_blocks)
            owner = lax.div(within, own_blocks)
            table_s[0, g, p] = lax.div(block, slab_blocks)
            table_s[1, g, p] = lax.rem(owner, 2)
            table_s[2, g, p] = lax.div(owner, 2) * own_blocks + lax.rem(within, own_blocks)
            table_s[3, g, p] = lax.div(within, groups)
            table_s[4, g, p] = lax.rem(within, groups)

    load_root.wait()
    for i in range(cols):
        start = pl.multiple_of((i * 2 + space) * own, own)
        upper, lower = split(root_v[pl.ds(start, own), :])
        left_s[0, i * own : (i + 1) * own] = upper
        left_s[1, i * own : (i + 1) * own] = lower
    for b in range(3):
        wide_hi[1, b], wide_lo[1, b] = split(root_v[:, b * slab : (b + 1) * slab])
        start = pl.multiple_of(b * slab + chunk * col, chunk)
        upper, lower = split(root_v[:, pl.ds(start, chunk)])
        near_hi[1, :, b * chunk : (b + 1) * chunk] = upper
        near_lo[1, :, b * chunk : (b + 1) * chunk] = lower

    relayed = {}
    gathers = {}

    def arrive(piece):
        pieces[piece].wait_recv()
        relayed[piece] = send(land(piece, col), land(piece, col), mate)

    def offer(piece):
        gathers[piece] = [
            send(land(piece, col), land(piece, col), side),
            send(land(piece, col), land(piece, col), cross),
        ]

    def half_rows(k, part):
        return ham_v.at[k, pl.ds(part * (own // 2), own // 2), :]

    arrive(0)
    arrive(2)
    ham_first.wait_recv()
    ham_half_a = send(half_rows(first, 1), half_rows(first, 1), cross)
    ham_second.wait_recv()
    ham_half_b = send(half_rows(second, 0), half_rows(second, 0), side)
    offer(0)
    offer(2)
    arrive(1)
    arrive(3)
    offer(1)
    offer(3)
    for piece in order_of_pieces:
        relayed[piece].wait_recv()
        upper, lower = split(land_v[piece // 2, piece % 2, :, lanes])
        side_of = 0 if piece < 2 else 2
        place = (0, 1, 1, 0)[piece]
        near_hi[side_of, :, place * chunk : (place + 1) * chunk] = upper
        near_lo[side_of, :, place * chunk : (place + 1) * chunk] = lower

    load_ham.wait()
    strips = (col, first, second, third)
    half_up, half_down, half_mate = [], [], []
    for i, strip in enumerate(strips):
        if i == 3:
            ham_half_a.wait_recv()
            ham_half_b.wait_recv()
        stacked = stack(ham_v[strip])
        terms = []
        for a in range(3):
            width = 3 * chunk if a == 1 else 2 * chunk
            terms.append(
                product(
                    stacked[:, a * slab : (a + 1) * slab],
                    (near_hi[a, :, :width], near_lo[a, :, :width]),
                )
            )
        done = mask_a[strip] * combine(*terms, chunk)
        for b in range(3):
            half_v[1, b, strip, space] = done[:, b * chunk : (b + 1) * chunk]
        half_up.append(
            send(
                half_v.at[1, pl.ds(1, 2), strip, space],
                half_v.at[0, pl.ds(0, 2), strip, space],
                up,
            )
        )
        half_down.append(
            send(
                half_v.at[1, pl.ds(0, 2), strip, space],
                half_v.at[2, pl.ds(1, 2), strip, space],
                down,
            )
        )
        half_mate.append(
            send(half_v.at[1, :, strip, space], half_v.at[1, :, strip, space], mate)
        )

    def window_block(ref, a):
        picked = {0: (0, 1), 1: (0, 1, 2), 2: (1, 2)}[a]
        return split(
            jnp.concatenate([ref[a, b].reshape(slab, chunk) for b in picked], axis=1)
        )

    def left_block(a):
        return left_s[:, :, a * slab : (a + 1) * slab].reshape(2 * half, slab)

    for copy in half_mate:
        copy.wait_recv()
    acc_v[...] = product(left_block(1), window_block(half_v, 1))
    relays = []
    mates = []
    for i, piece in enumerate(order_of_pieces):
        half_up[i].wait_recv()
        region = half_v.at[0, pl.ds(0, 2), strips[i], space]
        half_mate.append(send(region, region, mate))
        half_down[i].wait_recv()
        region = half_v.at[2, pl.ds(1, 2), strips[i], space]
        half_mate.append(send(region, region, mate))
        gathers[piece][0].wait_recv()
        relays.append(send(land(piece, first, 1), land(piece, first, 1), cross))
        mates.append(send(land(piece, first), land(piece, first), mate))
        gathers[piece][1].wait_recv()
        relays.append(send(land(piece, second, 0), land(piece, second, 0), side))
        mates.append(send(land(piece, second), land(piece, second), mate))
    for copy in half_mate[cols:]:
        copy.wait_recv()

    done = combine(
        product(left_block(0), window_block(half_v, 0)),
        acc_v[...],
        product(left_block(2), window_block(half_v, 2)),
        chunk,
    )
    for b in range(3):
        masked = mask_a[:, :, b * chunk : (b + 1) * chunk].reshape(half, chunk)
        masked = masked * done[:, b * chunk : (b + 1) * chunk]
        ortho_v[1, b, space, :, col] = masked.reshape(half // BLK, BLK, chunk)

    spans = {0: (0, 2), 1: (0, 3), 2: (1, 2)}

    def region(a, k, part=None, span=None):
        size = half // BLK if part is None else half // BLK // 2
        start = 0 if part is None else part * size
        return ortho_v.at[a, pl.ds(*(span or spans[a])), space, pl.ds(start, size), k]

    def pass_on(a, k, part, device):
        return send(region(a, k, part), region(a, k, part), device)

    def to_rows(k, part):
        return (
            send(region(1, k, part, (1, 2)), region(0, k, part), up),
            send(region(1, k, part, (0, 2)), region(2, k, part), down),
        )

    pending = []
    own_rows_out = to_rows(col, None)
    own_first = pass_on(1, col, None, side)
    own_second = pass_on(1, col, None, cross)
    pending.append(pass_on(1, col, None, mate))
    for copy in relays:
        copy.wait_recv()
    for piece in order_of_pieces:
        mates.append(send(land(piece, third), land(piece, third), mate))
    for copy in mates:
        copy.wait_recv()
    for piece in order_of_pieces:
        a = 0 if piece < 2 else 2
        b = (0, 1, 2, 1)[piece]
        wide_hi[a, b], wide_lo[a, b] = split(land_v[piece // 2, piece % 2])

    own_first.wait_recv()
    diagonal_a = pass_on(1, first, 1, cross)
    first_rows = to_rows(first, 0)
    pending.append(pass_on(1, first, None, mate))
    own_second.wait_recv()
    diagonal_b = pass_on(1, second, 0, side)
    second_rows = to_rows(second, 1)
    pending.append(pass_on(1, second, None, mate))
    hops = []
    for a, copy in ((0, own_rows_out[0]), (2, own_rows_out[1])):
        copy.wait_recv()
        hops.append((a, first, 1, pass_on(a, col, 1, side)))
        hops.append((a, second, 0, pass_on(a, col, 0, cross)))
        pending.append(pass_on(a, col, None, mate))
    diagonal_a.wait_recv()
    diagonal_b.wait_recv()
    pending.append(pass_on(1, third, None, mate))
    for a, copy in ((0, first_rows[0]), (2, first_rows[1])):
        copy.wait_recv()
        hops.append((a, third, 0, pass_on(a, first, 0, cross)))
        pending.append(pass_on(a, first, 0, mate))
    for a, copy in ((0, second_rows[0]), (2, second_rows[1])):
        copy.wait_recv()
        hops.append((a, third, 1, pass_on(a, second, 1, side)))
        pending.append(pass_on(a, second, 1, mate))
    for a, k, part, copy in hops:
        copy.wait_recv()
        pending.append(pass_on(a, k, part, mate))
    for copy in pending:
        copy.wait_recv()

    lane_group = lax.broadcasted_iota(jnp.int32, (8, chunk), 1) // BLK

    def solve(g):
        live = count_ref[g]

        for p in range(maxb):
            sub = table_s[4, g, p]
            steps = lax.rem(p + groups - sub, groups)
            turns_v[p] = jnp.where(
                lane_group == jnp.full(lane_group.shape, sub, jnp.int32),
                jnp.full(lane_group.shape, steps, jnp.int32),
                -1,
            )

        def assemble(i, inner):
            a, core, place = (table_s[field, g, i] for field in range(3))
            for t in range(maxb // groups):
                sorted_by = [jnp.zeros((BLK, chunk), F32)] * groups
                for e in range(groups):
                    p = t * groups + e
                    value = ortho_v[a, table_s[0, g, p], core, place, table_s[3, g, p]]
                    needed = jnp.tile(turns_v[p], (BLK // 8, 1))
                    for steps in range(groups):
                        sorted_by[steps] = jnp.where(needed == steps, value, sorted_by[steps])
                tile = sorted_by[0]
                for steps in range(1, groups):
                    tile = tile + pltpu.roll(sorted_by[steps], steps * BLK, 1)
                sub_v[pl.ds(pl.multiple_of(i * BLK, BLK), BLK), t * chunk : (t + 1) * chunk] = tile
            return inner

        lax.fori_loop(0, maxb, assemble, 0, unroll=2)
        position = [lax.broadcasted_iota(jnp.int32, (order, order), d) for d in range(2)]
        assembled = jnp.where(jnp.maximum(*position) < live * BLK, sub_v[...], 0.0)
        symmetric = 0.5 * (assembled + assembled.T)
        total = jnp.sum(jnp.sum(symmetric * symmetric, axis=1, keepdims=True), axis=0, keepdims=True)
        live_order = jnp.full((1, 1), live * BLK, jnp.int32).astype(F32)
        iterate = symmetric * (jnp.sqrt(live_order) / (2.0 * jnp.sqrt(total + 1e-06)))
        parts = split(iterate)
        square = split(dot(parts[0], parts[0]) + dot(parts[0], parts[1]) + dot(parts[1], parts[0]))

        def times_square(value):
            return product(stack(value), square)

        home = iterate[:BLK]
        home = 1.5 * home - 0.5 * times_square(home)
        cube = times_square(home)
        cube = 1.5 * cube - 0.5 * times_square(cube)
        cube = 1.5 * cube - 0.5 * times_square(cube)
        home = 1.5 * home - 0.5 * cube
        diagonal = lax.broadcasted_iota(jnp.int32, (BLK, order), 0) == lax.broadcasted_iota(
            jnp.int32, (BLK, order), 1
        )
        home = 0.5 * (jnp.where(diagonal, 1.0, 0.0) - home)
        tiles = [jnp.zeros((BLK, chunk), F32) for _ in range(window // chunk)]
        turned = [
            [home[:, t * chunk : (t + 1) * chunk]]
            + [
                pltpu.roll(home[:, t * chunk : (t + 1) * chunk], steps * BLK, 1)
                for steps in range(1, groups)
            ]
            for t in range(maxb // groups)
        ]
        for p in range(maxb):
            other = pos_ref[g, p]
            sub = lax.rem(other, groups)
            here = (lane_group == jnp.full(lane_group.shape, sub, jnp.int32)) & (
                jnp.full(lane_group.shape, live, jnp.int32) > p
            )
            place = jnp.where(
                here, jnp.full(lane_group.shape, lax.div(other, groups), jnp.int32), -1
            )
            place = jnp.tile(place, (BLK // 8, 1))
            ways = turned[p // groups]
            wide = jnp.tile(lane_group, (BLK // 8, 1))
            value = ways[(groups - p) % groups]
            for target in range(1, groups):
                value = jnp.where(wide == target, ways[(target + groups - p) % groups], value)
            for m in range(len(tiles)):
                tiles[m] = jnp.where(place == m, value, tiles[m])
        return jnp.concatenate(tiles, axis=1)

    def lanes_of(k):
        return pl.ds(pl.multiple_of(chunk * k, chunk), chunk)

    back_mate = []
    back = {
        (a, g, offset): []
        for a in (1, 0, 2)
        for g in range(own_blocks)
        for offset in (2, 1, 3, 0)
        if a != 1 or offset
    }
    for g in range(own_blocks):
        stacked = stack(solve(g))
        these = pl.ds(g * BLK, BLK)
        for b in (1, 0, 2):
            total = None
            for a in (0, 1, 2):
                if abs(a - b) > 1:
                    continue
                term = product(
                    stacked[:, a * slab : (a + 1) * slab], (wide_hi[a, b], wide_lo[a, b])
                )
                total = term if total is None else total + term
            rows_v[b, these] = mask_b[these, b * slab : (b + 1) * slab] * total
            for offset in (2, 1, 3, 0):
                target = lax.rem(col + offset, cols)
                source = rows_v.at[b, these, lanes_of(target)]
                if b > 0:
                    target_ref = back_v.at[0, b - 1, col, space, these]
                    device = {"rows": above, "cols": target}
                    back[0, g, offset].append(send(source, target_ref, device))
                if b < 2:
                    target_ref = back_v.at[2, b + 1, col, space, these]
                    device = {"rows": below, "cols": target}
                    back[2, g, offset].append(send(source, target_ref, device))
            for offset in (2, 1, 3):
                target = lax.rem(col + offset, cols)
                source = rows_v.at[b, these, lanes_of(target)]
                target_ref = back_v.at[1, b, col, space, these]
                back[1, g, offset].append(send(source, target_ref, {"cols": target}))
        back_mate.append(
            send(rows_v.at[:, these, lanes], back_v.at[1, :, col, space, these], mate)
        )
    back_v[1, :, col, space] = rows_v[:, :, lanes]
    for (a, g, offset), copies in sorted(
        back.items(), key=lambda item: (item[0][0] != 1, item[0][1])
    ):
        for copy in copies:
            copy.wait_recv()
        origin = lax.rem(col + cols - offset, cols)
        piece = back_v.at[a, pl.ds(*spans[a]), origin, space, pl.ds(g * BLK, BLK)]
        back_mate.append(send(piece, piece, mate))
        if len(back_mate) == own_blocks * cols:
            for other in back_mate:
                other.wait_recv()
            acc_v[...] = product(left_block(1), window_block(back_v, 1))
    for other in back_mate[own_blocks * cols :]:
        other.wait_recv()
    done = combine(
        product(left_block(0), window_block(back_v, 0)),
        acc_v[...],
        product(left_block(2), window_block(back_v, 2)),
        chunk,
    )
    for b in range(3):
        masked = mask_a[:, :, b * chunk : (b + 1) * chunk].reshape(half, chunk)
        piece = masked * done[:, b * chunk : (b + 1) * chunk]
        strip_v[:, b] = piece.reshape(cols, own, chunk)
    outs = []
    for offset in (2, 1, 3):
        target = lax.rem(col + offset, cols)
        outs.append(send(strip_v.at[target], final_v.at[col], {"cols": target}))
    final_v[col] = strip_v[col]
    for copy in outs:
        copy.wait_recv()
    total = jnp.zeros((own, chunk), F32)
    for b in range(3):
        for k in range(cols):
            value = final_v[k, b]
            total = total + value
            density_ref[:, b * slab + k * chunk : b * slab + (k + 1) * chunk] = value
    charges_ref[...] = jnp.sum(total.T, axis=0)
    send.finish()


def place_kernel(density_ref, charges_ref, density_out, charges_out, density_v, charges_v, sems):
    inward = [
        pltpu.make_async_copy(density_ref, density_v, sems.at[0]),
        pltpu.make_async_copy(charges_ref, charges_v, sems.at[1]),
    ]
    outward = [
        pltpu.make_async_copy(density_v, density_out, sems.at[2]),
        pltpu.make_async_copy(charges_v, charges_out, sems.at[3]),
    ]
    for copy in inward:
        copy.start()
    for copy, then in zip(inward, outward):
        copy.wait()
        then.start()
    for copy in outward:
        copy.wait()


def shards(hamiltonian, correlation_root, pattern, sub_blocks, sub_count):
    slab, window = correlation_root.shape
    own = hamiltonian.shape[0]
    cols = lax.axis_size("cols")
    chunk = slab // cols
    half = slab // 2
    own_blocks, maxb = sub_blocks.shape
    order = maxb * BLK
    vmem = functools.partial(pltpu.VMEM)
    density, charges = pl.pallas_call(
        kernel,
        out_shape=[
            jax.ShapeDtypeStruct((own, window), F32),
            jax.ShapeDtypeStruct((own,), F32),
        ],
        in_specs=[
            pl.BlockSpec(memory_space=pltpu.HBM),
        ]
        * 5,
        out_specs=[pl.BlockSpec(memory_space=pltpu.VMEM)] * 2,
        scratch_shapes=[
            vmem((slab, window), F32),
            vmem((2, half, window), BF16),
            vmem((cols, own, window), F32),
            vmem((2, 2, slab, slab), F32),
            vmem((3, 3, slab, slab), BF16),
            vmem((3, 3, slab, slab), BF16),
            vmem((3, slab, 3 * chunk), BF16),
            vmem((3, slab, 3 * chunk), BF16),
            vmem((cols, own, 3 * chunk), F32),
            vmem((own, window), F32),
            vmem((3, 3, cols, 2, own, chunk), F32),
            vmem((3, 3, cols, 2, own, chunk), F32),
            vmem((3, 3, 2, half // BLK, cols, BLK, chunk), F32),
            vmem((half, 3 * chunk), F32),
            vmem((order, order), F32),
            vmem((maxb, 8, chunk), jnp.int32),
            vmem((3, own, slab), F32),
            vmem((cols, 3, own, chunk), F32),
            vmem((cols, 3, own, chunk), F32),
            pltpu.VMEM(pattern.T.shape, jnp.int32),
            pltpu.SMEM(sub_blocks.shape, jnp.int32),
            pltpu.SMEM(sub_count.shape, jnp.int32),
            pltpu.SMEM((5, own_blocks, maxb), jnp.int32),
            pltpu.SemaphoreType.DMA((5,)),
            pltpu.SemaphoreType.DMA((240,)),
            pltpu.SemaphoreType.DMA((240,)),
        ],
        compiler_params=pltpu.CompilerParams(
            collective_id=1, has_side_effects=True, vmem_limit_bytes=62 * 2**20
        ),
    )(sub_blocks, sub_count, hamiltonian, correlation_root, pattern.T)
    return pl.pallas_call(
        place_kernel,
        out_shape=[
            jax.ShapeDtypeStruct((own, window), F32),
            jax.ShapeDtypeStruct((own,), F32),
        ],
        in_specs=[pl.BlockSpec(memory_space=pltpu.HBM)] * 2,
        out_specs=[pl.BlockSpec(memory_space=pltpu.HBM)] * 2,
        scratch_shapes=[
            pltpu.VMEM((own, window), F32),
            pltpu.VMEM((own,), F32),
            pltpu.SemaphoreType.DMA((4,)),
        ],
        compiler_params=pltpu.CompilerParams(vmem_limit_bytes=62 * 2**20),
    )(density, charges)


def solution(mesh):
    return jax.shard_map(
        shards,
        mesh=mesh,
        in_specs=(
            P(("rows", "cols", "space"), None),
            P("rows", None),
            P(),
            P(("rows", "cols", "space"), None),
            P(("rows", "cols", "space")),
        ),
        out_specs=(P(("rows", "cols", "space"), None), P(("rows", "cols", "space"))),
        check_vma=False,
    )
```

```python
import functools

import jax
import jax.numpy as jnp
from jax import lax
from jax.experimental import pallas as pl
from jax.experimental.pallas import tpu as pltpu
from jax.sharding import PartitionSpec as P

BLK = 32
F32 = jnp.float32
BF16 = jnp.bfloat16


def split(value):
    upper = value.astype(BF16)
    return upper, (value - upper.astype(F32)).astype(BF16)


def dot(leftside, rightside):
    return jnp.dot(leftside, rightside, preferred_element_type=F32)


def product(stacked, right):
    high, low = right
    half = stacked.shape[0] // 2
    both = dot(stacked, high)
    return both[:half] + both[half:] + dot(stacked[:half], low)


def stack(value):
    return jnp.concatenate(split(value), axis=0)


def combine(above, own, below, width):
    return jnp.concatenate(
        [
            above[:, :width] + own[:, :width],
            above[:, width:] + own[:, width : 2 * width] + below[:, :width],
            own[:, 2 * width :] + below[:, width:],
        ],
        axis=1,
    )


class Sender:
    def __init__(self, send_sems, recv_sems):
        self.sems = (send_sems, recv_sems)
        self.copies = []

    def __call__(self, source, target, device):
        slot = len(self.copies)
        copy = pltpu.make_async_remote_copy(
            src_ref=source,
            dst_ref=target,
            send_sem=self.sems[0].at[slot],
            recv_sem=self.sems[1].at[slot],
            device_id=device,
            device_id_type=pl.DeviceIdType.MESH,
        )
        copy.start()
        self.copies.append(copy)
        return copy

    def finish(self):
        for copy in self.copies:
            copy.wait_send()


def kernel(
    pos_in,
    count_in,
    ham_ref,
    root_ref,
    pattern_in,
    density_ref,
    charges_ref,
    root_v,
    left_s,
    ham_v,
    land_v,
    wide_hi,
    wide_lo,
    near_hi,
    near_lo,
    mask_a,
    mask_b,
    half_v,
    back_v,
    ortho_v,
    acc_v,
    sub_v,
    turns_v,
    rows_v,
    strip_v,
    final_v,
    pattern_ref,
    pos_ref,
    count_ref,
    table_s,
    local_sems,
    send_sems,
    recv_sems,
):
    row = lax.axis_index("rows")
    count = lax.axis_size("rows")
    col = lax.axis_index("cols")
    space = lax.axis_index("space")
    cols = lax.axis_size("cols")
    slab, window = root_v.shape
    own = ham_ref.shape[0]
    chunk = slab // cols
    half = slab // 2
    maxb = pos_ref.shape[1]
    slab_blocks = slab // BLK
    own_blocks = own // BLK
    order = maxb * BLK
    groups = chunk // BLK

    first = col + 1 - 2 * lax.rem(col, 2)
    second = lax.rem(col + 2, 4)
    third = lax.rem(first + 2, 4)
    above = lax.rem(row + 1, count)
    below = lax.rem(row + count - 1, count)
    up, down = {"rows": above}, {"rows": below}
    side, cross, mate = {"cols": first}, {"cols": second}, {"space": 1 - space}
    lanes = pl.ds(pl.multiple_of(chunk * col, chunk), chunk)

    load_root = pltpu.make_async_copy(root_ref, root_v, local_sems.at[0])
    load_ham = pltpu.make_async_copy(ham_ref, ham_v.at[col], local_sems.at[1])
    small = [
        pltpu.make_async_copy(pos_in, pos_ref, local_sems.at[2]),
        pltpu.make_async_copy(count_in, count_ref, local_sems.at[3]),
        pltpu.make_async_copy(pattern_in, pattern_ref, local_sems.at[4]),
    ]
    load_root.start()
    load_ham.start()
    for copy in small:
        copy.start()

    barrier = pltpu.get_barrier_semaphore()
    peers = [mate]
    for offset in range(cols):
        other = lax.rem(col + offset, cols)
        peers += [{"rows": above, "cols": other}, {"rows": below, "cols": other}]
        if offset:
            peers.append({"cols": other})
    for peer in peers:
        pl.semaphore_signal(barrier, inc=1, device_id=peer, device_id_type=pl.DeviceIdType.MESH)
    pl.semaphore_wait(barrier, len(peers))
    send = Sender(send_sems, recv_sems)

    ham_first = send(ham_ref, ham_v.at[col], side)
    ham_second = send(ham_ref, ham_v.at[col], cross)

    def land(piece, k, part=None):
        size = half if part is None else half // 2
        start = half * space + (0 if part is None else part * size)
        return land_v.at[
            piece // 2,
            piece % 2,
            pl.ds(pl.multiple_of(start, size), size),
            pl.ds(pl.multiple_of(chunk * k, chunk), chunk),
        ]

    order_of_pieces = (0, 2, 1, 3)
    pieces = {}
    for piece in order_of_pieces:
        panel = (1, 2, 1, 0)[piece]
        source = root_ref.at[
            pl.ds(pl.multiple_of(half * space, half), half),
            pl.ds(pl.multiple_of(panel * slab + chunk * col, chunk), chunk),
        ]
        pieces[piece] = send(source, land(piece, col), up if piece < 2 else down)

    zero = jnp.zeros(ortho_v.shape[3:], F32)
    for part in range(2):
        ortho_v[0, 2, part] = zero
        ortho_v[2, 0, part] = zero

    for copy in small:
        copy.wait()
    pattern = pattern_ref[...].astype(F32).astype(BF16)
    blocks_all = pattern.shape[1]

    def pick(rows, block_of):
        wanted = block_of(lax.broadcasted_iota(jnp.int32, (rows, blocks_all), 0))
        here = lax.broadcasted_iota(jnp.int32, (rows, blocks_all), 1)
        chosen = jnp.where(wanted == here, 1.0, 0.0).astype(BF16)
        return lax.dot_general(
            chosen, pattern, (((1,), (1,)), ((), ())), preferred_element_type=F32
        ).astype(BF16)

    def spread(values, wanted):
        here = lax.broadcasted_iota(jnp.int32, wanted.shape, 0)
        return dot(values, jnp.where(wanted == here, 1.0, 0.0).astype(BF16))

    base = row * slab_blocks
    strip_rows = pick(
        cols * own,
        lambda i: base + ((i // own) * 2 + space) * own_blocks + (i % own) // BLK,
    )
    lane = lax.broadcasted_iota(jnp.int32, (3 * slab_blocks, 3 * chunk), 1)
    chip_mask = spread(
        strip_rows, (lane // chunk) * slab_blocks + col * groups + (lane % chunk) // BLK
    )
    for i in range(cols):
        mask_a[i] = chip_mask[i * own : (i + 1) * own]
    own_rows = pick(own, lambda i: base + (col * 2 + space) * own_blocks + i // BLK)
    lane = lax.broadcasted_iota(jnp.int32, (3 * slab_blocks, window), 1)
    mask_b[...] = spread(own_rows, lane // BLK)

    for g in range(own_blocks):
        for p in range(maxb):
            block = pos_ref[g, p]
            within = lax.rem(block, slab_blocks)
            owner = lax.div(within, own_blocks)
            table_s[0, g, p] = lax.div(block, slab_blocks)
            table_s[1, g, p] = lax.rem(owner, 2)
            table_s[2, g, p] = lax.div(owner, 2) * own_blocks + lax.rem(within, own_blocks)
            table_s[3, g, p] = lax.div(within, groups)
            table_s[4, g, p] = lax.rem(within, groups)

    load_root.wait()
    for i in range(cols):
        start = pl.multiple_of((i * 2 + space) * own, own)
        upper, lower = split(root_v[pl.ds(start, own), :])
        left_s[0, i * own : (i + 1) * own] = upper
        left_s[1, i * own : (i + 1) * own] = lower
    for b in range(3):
        wide_hi[1, b], wide_lo[1, b] = split(root_v[:, b * slab : (b + 1) * slab])
        start = pl.multiple_of(b * slab + chunk * col, chunk)
        upper, lower = split(root_v[:, pl.ds(start, chunk)])
        near_hi[1, :, b * chunk : (b + 1) * chunk] = upper
        near_lo[1, :, b * chunk : (b + 1) * chunk] = lower

    relayed = {}
    gathers = {}

    def arrive(piece):
        pieces[piece].wait_recv()
        relayed[piece] = send(land(piece, col), land(piece, col), mate)

    def offer(piece):
        gathers[piece] = [
            send(land(piece, col), land(piece, col), side),
            send(land(piece, col), land(piece, col), cross),
        ]

    def half_rows(k, part):
        return ham_v.at[k, pl.ds(part * (own // 2), own // 2), :]

    arrive(0)
    arrive(2)
    ham_first.wait_recv()
    ham_half_a = send(half_rows(first, 1), half_rows(first, 1), cross)
    ham_second.wait_recv()
    ham_half_b = send(half_rows(second, 0), half_rows(second, 0), side)
    offer(0)
    offer(2)
    arrive(1)
    arrive(3)
    offer(1)
    offer(3)
    for piece in order_of_pieces:
        relayed[piece].wait_recv()
        upper, lower = split(land_v[piece // 2, piece % 2, :, lanes])
        side_of = 0 if piece < 2 else 2
        place = (0, 1, 1, 0)[piece]
        near_hi[side_of, :, place * chunk : (place + 1) * chunk] = upper
        near_lo[side_of, :, place * chunk : (place + 1) * chunk] = lower

    load_ham.wait()
    strips = (col, first, second, third)
    half_up, half_down, half_mate = [], [], []
    for i, strip in enumerate(strips):
        if i == 3:
            ham_half_a.wait_recv()
            ham_half_b.wait_recv()
        stacked = stack(ham_v[strip])
        terms = []
        for a in range(3):
            width = 3 * chunk if a == 1 else 2 * chunk
            terms.append(
                product(
                    stacked[:, a * slab : (a + 1) * slab],
                    (near_hi[a, :, :width], near_lo[a, :, :width]),
                )
            )
        done = mask_a[strip] * combine(*terms, chunk)
        for b in range(3):
            half_v[1, b, strip, space] = done[:, b * chunk : (b + 1) * chunk]
        half_up.append(
            send(
                half_v.at[1, pl.ds(1, 2), strip, space],
                half_v.at[0, pl.ds(0, 2), strip, space],
                up,
            )
        )
        half_down.append(
            send(
                half_v.at[1, pl.ds(0, 2), strip, space],
                half_v.at[2, pl.ds(1, 2), strip, space],
                down,
            )
        )
        half_mate.append(
            send(half_v.at[1, :, strip, space], half_v.at[1, :, strip, space], mate)
        )

    def window_block(ref, a):
        picked = {0: (0, 1), 1: (0, 1, 2), 2: (1, 2)}[a]
        return split(
            jnp.concatenate([ref[a, b].reshape(slab, chunk) for b in picked], axis=1)
        )

    def left_block(a):
        return left_s[:, :, a * slab : (a + 1) * slab].reshape(2 * half, slab)

    for copy in half_mate:
        copy.wait_recv()
    acc_v[...] = product(left_block(1), window_block(half_v, 1))
    relays = []
    mates = []
    for i, piece in enumerate(order_of_pieces):
        half_up[i].wait_recv()
        region = half_v.at[0, pl.ds(0, 2), strips[i], space]
        half_mate.append(send(region, region, mate))
        half_down[i].wait_recv()
        region = half_v.at[2, pl.ds(1, 2), strips[i], space]
        half_mate.append(send(region, region, mate))
        gathers[piece][0].wait_recv()
        relays.append(send(land(piece, first, 1), land(piece, first, 1), cross))
        mates.append(send(land(piece, first), land(piece, first), mate))
        gathers[piece][1].wait_recv()
        relays.append(send(land(piece, second, 0), land(piece, second, 0), side))
        mates.append(send(land(piece, second), land(piece, second), mate))
    for copy in half_mate[cols:]:
        copy.wait_recv()

    done = combine(
        product(left_block(0), window_block(half_v, 0)),
        acc_v[...],
        product(left_block(2), window_block(half_v, 2)),
        chunk,
    )
    for b in range(3):
        masked = mask_a[:, :, b * chunk : (b + 1) * chunk].reshape(half, chunk)
        masked = masked * done[:, b * chunk : (b + 1) * chunk]
        ortho_v[1, b, space, :, col] = masked.reshape(half // BLK, BLK, chunk)

    spans = {0: (0, 2), 1: (0, 3), 2: (1, 2)}

    def region(a, k, b, part=None):
        size = half // BLK if part is None else half // BLK // 2
        start = 0 if part is None else part * size
        return ortho_v.at[a, b, space, pl.ds(start, size), k]

    def pass_on(a, k, b, part, device):
        return send(region(a, k, b, part), region(a, k, b, part), device)

    def to_rows(k, b, part):
        copies = []
        if b > 0:
            copies.append((0, b - 1, send(region(1, k, b, part), region(0, k, b - 1, part), up)))
        if b < 2:
            copies.append((2, b + 1, send(region(1, k, b, part), region(2, k, b + 1, part), down)))
        return copies

    panels = (1, 0, 2)
    pending = []
    own_rows_out, own_first, own_second = {}, {}, {}
    for b in panels:
        own_rows_out[b] = to_rows(col, b, None)
        own_first[b] = pass_on(1, col, b, None, side)
        own_second[b] = pass_on(1, col, b, None, cross)
        pending.append(pass_on(1, col, b, None, mate))
    for copy in relays:
        copy.wait_recv()
    for piece in order_of_pieces:
        mates.append(send(land(piece, third), land(piece, third), mate))
    for copy in mates:
        copy.wait_recv()
    for piece in order_of_pieces:
        a = 0 if piece < 2 else 2
        b = (0, 1, 2, 1)[piece]
        wide_hi[a, b], wide_lo[a, b] = split(land_v[piece // 2, piece % 2])

    hops, diagonals, first_rows, second_rows = [], {}, {}, {}
    for b in panels:
        own_first[b].wait_recv()
        first_rows[b] = to_rows(first, b, 0)
        diagonal_a = pass_on(1, first, b, 1, cross)
        pending.append(pass_on(1, first, b, None, mate))
        own_second[b].wait_recv()
        second_rows[b] = to_rows(second, b, 1)
        diagonals[b] = (diagonal_a, pass_on(1, second, b, 0, side))
        pending.append(pass_on(1, second, b, None, mate))
        for a, place, copy in own_rows_out[b]:
            copy.wait_recv()
            hops.append((a, first, place, 1, pass_on(a, col, place, 1, side)))
            hops.append((a, second, place, 0, pass_on(a, col, place, 0, cross)))
            pending.append(pass_on(a, col, place, None, mate))
    for b in panels:
        for copy in diagonals[b]:
            copy.wait_recv()
        pending.append(pass_on(1, third, b, None, mate))
        for a, place, copy in first_rows[b]:
            copy.wait_recv()
            hops.append((a, third, place, 0, pass_on(a, first, place, 0, cross)))
            pending.append(pass_on(a, first, place, 0, mate))
        for a, place, copy in second_rows[b]:
            copy.wait_recv()
            hops.append((a, third, place, 1, pass_on(a, second, place, 1, side)))
            pending.append(pass_on(a, second, place, 1, mate))
    for a, k, place, part, copy in hops:
        copy.wait_recv()
        pending.append(pass_on(a, k, place, part, mate))
    for copy in pending:
        copy.wait_recv()

    lane_group = lax.broadcasted_iota(jnp.int32, (8, chunk), 1) // BLK

    def solve(g):
        live = count_ref[g]

        for p in range(maxb):
            sub = table_s[4, g, p]
            steps = lax.rem(p + groups - sub, groups)
            turns_v[p] = jnp.where(
                lane_group == jnp.full(lane_group.shape, sub, jnp.int32),
                jnp.full(lane_group.shape, steps, jnp.int32),
                -1,
            )

        def assemble(i, inner):
            a, core, place = (table_s[field, g, i] for field in range(3))
            for t in range(maxb // groups):
                sorted_by = [jnp.zeros((BLK, chunk), F32)] * groups
                for e in range(groups):
                    p = t * groups + e
                    value = ortho_v[a, table_s[0, g, p], core, place, table_s[3, g, p]]
                    needed = jnp.tile(turns_v[p], (BLK // 8, 1))
                    for steps in range(groups):
                        sorted_by[steps] = jnp.where(needed == steps, value, sorted_by[steps])
                tile = sorted_by[0]
                for steps in range(1, groups):
                    tile = tile + pltpu.roll(sorted_by[steps], steps * BLK, 1)
                sub_v[pl.ds(pl.multiple_of(i * BLK, BLK), BLK), t * chunk : (t + 1) * chunk] = tile
            return inner

        lax.fori_loop(0, maxb, assemble, 0, unroll=2)
        position = [lax.broadcasted_iota(jnp.int32, (order, order), d) for d in range(2)]
        assembled = jnp.where(jnp.maximum(*position) < live * BLK, sub_v[...], 0.0)
        symmetric = 0.5 * (assembled + assembled.T)
        total = jnp.sum(jnp.sum(symmetric * symmetric, axis=1, keepdims=True), axis=0, keepdims=True)
        live_order = jnp.full((1, 1), live * BLK, jnp.int32).astype(F32)
        iterate = symmetric * (jnp.sqrt(live_order) / (2.0 * jnp.sqrt(total + 1e-06)))
        parts = split(iterate)
        square = split(dot(parts[0], parts[0]) + dot(parts[0], parts[1]) + dot(parts[1], parts[0]))

        def times_square(value):
            return product(stack(value), square)

        home = iterate[:BLK]
        home = 1.5 * home - 0.5 * times_square(home)
        cube = times_square(home)
        cube = 1.5 * cube - 0.5 * times_square(cube)
        cube = 1.5 * cube - 0.5 * times_square(cube)
        home = 1.5 * home - 0.5 * cube
        diagonal = lax.broadcasted_iota(jnp.int32, (BLK, order), 0) == lax.broadcasted_iota(
            jnp.int32, (BLK, order), 1
        )
        home = 0.5 * (jnp.where(diagonal, 1.0, 0.0) - home)
        tiles = [jnp.zeros((BLK, chunk), F32) for _ in range(window // chunk)]
        turned = [
            [home[:, t * chunk : (t + 1) * chunk]]
            + [
                pltpu.roll(home[:, t * chunk : (t + 1) * chunk], steps * BLK, 1)
                for steps in range(1, groups)
            ]
            for t in range(maxb // groups)
        ]
        for p in range(maxb):
            other = pos_ref[g, p]
            sub = lax.rem(other, groups)
            here = (lane_group == jnp.full(lane_group.shape, sub, jnp.int32)) & (
                jnp.full(lane_group.shape, live, jnp.int32) > p
            )
            place = jnp.where(
                here, jnp.full(lane_group.shape, lax.div(other, groups), jnp.int32), -1
            )
            place = jnp.tile(place, (BLK // 8, 1))
            ways = turned[p // groups]
            wide = jnp.tile(lane_group, (BLK // 8, 1))
            value = ways[(groups - p) % groups]
            for target in range(1, groups):
                value = jnp.where(wide == target, ways[(target + groups - p) % groups], value)
            for m in range(len(tiles)):
                tiles[m] = jnp.where(place == m, value, tiles[m])
        return jnp.concatenate(tiles, axis=1)

    def lanes_of(k):
        return pl.ds(pl.multiple_of(chunk * k, chunk), chunk)

    back_mate = []
    back = {
        (a, g, offset): []
        for a in (1, 0, 2)
        for g in range(own_blocks)
        for offset in (2, 1, 3, 0)
        if a != 1 or offset
    }
    for g in range(own_blocks):
        stacked = stack(solve(g))
        these = pl.ds(g * BLK, BLK)
        for b in (1, 0, 2):
            total = None
            for a in (0, 1, 2):
                if abs(a - b) > 1:
                    continue
                term = product(
                    stacked[:, a * slab : (a + 1) * slab], (wide_hi[a, b], wide_lo[a, b])
                )
                total = term if total is None else total + term
            rows_v[b, these] = mask_b[these, b * slab : (b + 1) * slab] * total
            for offset in (2, 1, 3, 0):
                target = lax.rem(col + offset, cols)
                source = rows_v.at[b, these, lanes_of(target)]
                if b > 0:
                    target_ref = back_v.at[0, b - 1, col, space, these]
                    device = {"rows": above, "cols": target}
                    back[0, g, offset].append(send(source, target_ref, device))
                if b < 2:
                    target_ref = back_v.at[2, b + 1, col, space, these]
                    device = {"rows": below, "cols": target}
                    back[2, g, offset].append(send(source, target_ref, device))
            for offset in (2, 1, 3):
                target = lax.rem(col + offset, cols)
                source = rows_v.at[b, these, lanes_of(target)]
                target_ref = back_v.at[1, b, col, space, these]
                back[1, g, offset].append(send(source, target_ref, {"cols": target}))
        back_mate.append(
            send(rows_v.at[:, these, lanes], back_v.at[1, :, col, space, these], mate)
        )
    back_v[1, :, col, space] = rows_v[:, :, lanes]
    for (a, g, offset), copies in sorted(
        back.items(), key=lambda item: (item[0][0] != 1, item[0][1])
    ):
        for copy in copies:
            copy.wait_recv()
        origin = lax.rem(col + cols - offset, cols)
        piece = back_v.at[a, pl.ds(*spans[a]), origin, space, pl.ds(g * BLK, BLK)]
        back_mate.append(send(piece, piece, mate))
        if len(back_mate) == own_blocks * cols:
            for other in back_mate:
                other.wait_recv()
            acc_v[...] = product(left_block(1), window_block(back_v, 1))
    for other in back_mate[own_blocks * cols :]:
        other.wait_recv()
    done = combine(
        product(left_block(0), window_block(back_v, 0)),
        acc_v[...],
        product(left_block(2), window_block(back_v, 2)),
        chunk,
    )
    for b in range(3):
        masked = mask_a[:, :, b * chunk : (b + 1) * chunk].reshape(half, chunk)
        piece = masked * done[:, b * chunk : (b + 1) * chunk]
        strip_v[:, b] = piece.reshape(cols, own, chunk)
    outs = []
    for offset in (2, 1, 3):
        target = lax.rem(col + offset, cols)
        outs.append(send(strip_v.at[target], final_v.at[col], {"cols": target}))
    final_v[col] = strip_v[col]
    for copy in outs:
        copy.wait_recv()
    total = jnp.zeros((own, chunk), F32)
    for b in range(3):
        for k in range(cols):
            value = final_v[k, b]
            total = total + value
            density_ref[:, b * slab + k * chunk : b * slab + (k + 1) * chunk] = value
    charges_ref[...] = jnp.sum(total.T, axis=0)
    send.finish()


def place_kernel(density_ref, charges_ref, density_out, charges_out, density_v, charges_v, sems):
    inward = [
        pltpu.make_async_copy(density_ref, density_v, sems.at[0]),
        pltpu.make_async_copy(charges_ref, charges_v, sems.at[1]),
    ]
    outward = [
        pltpu.make_async_copy(density_v, density_out, sems.at[2]),
        pltpu.make_async_copy(charges_v, charges_out, sems.at[3]),
    ]
    for copy in inward:
        copy.start()
    for copy, then in zip(inward, outward):
        copy.wait()
        then.start()
    for copy in outward:
        copy.wait()


def shards(hamiltonian, correlation_root, pattern, sub_blocks, sub_count):
    slab, window = correlation_root.shape
    own = hamiltonian.shape[0]
    cols = lax.axis_size("cols")
    chunk = slab // cols
    half = slab // 2
    own_blocks, maxb = sub_blocks.shape
    order = maxb * BLK
    vmem = functools.partial(pltpu.VMEM)
    density, charges = pl.pallas_call(
        kernel,
        out_shape=[
            jax.ShapeDtypeStruct((own, window), F32),
            jax.ShapeDtypeStruct((own,), F32),
        ],
        in_specs=[
            pl.BlockSpec(memory_space=pltpu.HBM),
        ]
        * 5,
        out_specs=[pl.BlockSpec(memory_space=pltpu.VMEM)] * 2,
        scratch_shapes=[
            vmem((slab, window), F32),
            vmem((2, half, window), BF16),
            vmem((cols, own, window), F32),
            vmem((2, 2, slab, slab), F32),
            vmem((3, 3, slab, slab), BF16),
            vmem((3, 3, slab, slab), BF16),
            vmem((3, slab, 3 * chunk), BF16),
            vmem((3, slab, 3 * chunk), BF16),
            vmem((cols, own, 3 * chunk), F32),
            vmem((own, window), F32),
            vmem((3, 3, cols, 2, own, chunk), F32),
            vmem((3, 3, cols, 2, own, chunk), F32),
            vmem((3, 3, 2, half // BLK, cols, BLK, chunk), F32),
            vmem((half, 3 * chunk), F32),
            vmem((order, order), F32),
            vmem((maxb, 8, chunk), jnp.int32),
            vmem((3, own, slab), F32),
            vmem((cols, 3, own, chunk), F32),
            vmem((cols, 3, own, chunk), F32),
            pltpu.VMEM(pattern.T.shape, jnp.int32),
            pltpu.SMEM(sub_blocks.shape, jnp.int32),
            pltpu.SMEM(sub_count.shape, jnp.int32),
            pltpu.SMEM((5, own_blocks, maxb), jnp.int32),
            pltpu.SemaphoreType.DMA((5,)),
            pltpu.SemaphoreType.DMA((320,)),
            pltpu.SemaphoreType.DMA((320,)),
        ],
        compiler_params=pltpu.CompilerParams(
            collective_id=1, has_side_effects=True, vmem_limit_bytes=62 * 2**20
        ),
    )(sub_blocks, sub_count, hamiltonian, correlation_root, pattern.T)
    return pl.pallas_call(
        place_kernel,
        out_shape=[
            jax.ShapeDtypeStruct((own, window), F32),
            jax.ShapeDtypeStruct((own,), F32),
        ],
        in_specs=[pl.BlockSpec(memory_space=pltpu.HBM)] * 2,
        out_specs=[pl.BlockSpec(memory_space=pltpu.HBM)] * 2,
        scratch_shapes=[
            pltpu.VMEM((own, window), F32),
            pltpu.VMEM((own,), F32),
            pltpu.SemaphoreType.DMA((4,)),
        ],
        compiler_params=pltpu.CompilerParams(vmem_limit_bytes=62 * 2**20),
    )(density, charges)


def solution(mesh):
    return jax.shard_map(
        shards,
        mesh=mesh,
        in_specs=(
            P(("rows", "cols", "space"), None),
            P("rows", None),
            P(),
            P(("rows", "cols", "space"), None),
            P(("rows", "cols", "space")),
        ),
        out_specs=(P(("rows", "cols", "space"), None), P(("rows", "cols", "space"))),
        check_vma=False,
    )
```

```python
import functools

import jax
import jax.numpy as jnp
from jax import lax
from jax.experimental import pallas as pl
from jax.experimental.pallas import tpu as pltpu
from jax.sharding import PartitionSpec as P

BLK = 32
F32 = jnp.float32
BF16 = jnp.bfloat16


def split(value):
    upper = value.astype(BF16)
    return upper, (value - upper.astype(F32)).astype(BF16)


def dot(leftside, rightside):
    return jnp.dot(leftside, rightside, preferred_element_type=F32)


def product(stacked, right):
    high, low = right
    half = stacked.shape[0] // 2
    if half >= 256:
        return dot(stacked[:half], high) + dot(stacked[half:], high) + dot(stacked[:half], low)
    both = dot(stacked, high)
    return both[:half] + both[half:] + dot(stacked[:half], low)


def stack(value):
    return jnp.concatenate(split(value), axis=0)


def combine(above, own, below, width):
    return jnp.concatenate(
        [
            above[:, :width] + own[:, :width],
            above[:, width:] + own[:, width : 2 * width] + below[:, :width],
            own[:, 2 * width :] + below[:, width:],
        ],
        axis=1,
    )


class Sender:
    def __init__(self, send_sems, recv_sems):
        self.sems = (send_sems, recv_sems)
        self.copies = []

    def __call__(self, source, target, device):
        slot = len(self.copies)
        copy = pltpu.make_async_remote_copy(
            src_ref=source,
            dst_ref=target,
            send_sem=self.sems[0].at[slot],
            recv_sem=self.sems[1].at[slot],
            device_id=device,
            device_id_type=pl.DeviceIdType.MESH,
        )
        copy.start()
        self.copies.append(copy)
        return copy

    def finish(self):
        for copy in self.copies:
            copy.wait_send()


def kernel(
    pos_in,
    count_in,
    ham_ref,
    root_ref,
    pattern_in,
    density_ref,
    charges_ref,
    root_v,
    left_s,
    ham_v,
    land_v,
    wide_hi,
    wide_lo,
    near_hi,
    near_lo,
    mask_a,
    mask_b,
    half_v,
    back_v,
    ortho_v,
    acc_v,
    sub_v,
    turns_v,
    rows_v,
    strip_v,
    final_v,
    pattern_ref,
    pos_ref,
    count_ref,
    table_s,
    local_sems,
    send_sems,
    recv_sems,
):
    row = lax.axis_index("rows")
    count = lax.axis_size("rows")
    col = lax.axis_index("cols")
    space = lax.axis_index("space")
    cols = lax.axis_size("cols")
    slab, window = root_v.shape
    own = ham_ref.shape[0]
    chunk = slab // cols
    half = slab // 2
    maxb = pos_ref.shape[1]
    slab_blocks = slab // BLK
    own_blocks = own // BLK
    order = maxb * BLK
    groups = chunk // BLK

    first = col + 1 - 2 * lax.rem(col, 2)
    second = lax.rem(col + 2, 4)
    third = lax.rem(first + 2, 4)
    above = lax.rem(row + 1, count)
    below = lax.rem(row + count - 1, count)
    up, down = {"rows": above}, {"rows": below}
    side, cross, mate = {"cols": first}, {"cols": second}, {"space": 1 - space}
    lanes = pl.ds(pl.multiple_of(chunk * col, chunk), chunk)

    load_root = pltpu.make_async_copy(root_ref, root_v, local_sems.at[0])
    load_ham = pltpu.make_async_copy(ham_ref, ham_v.at[col], local_sems.at[1])
    small = [
        pltpu.make_async_copy(pos_in, pos_ref, local_sems.at[2]),
        pltpu.make_async_copy(count_in, count_ref, local_sems.at[3]),
        pltpu.make_async_copy(pattern_in, pattern_ref, local_sems.at[4]),
    ]
    load_root.start()
    load_ham.start()
    for copy in small:
        copy.start()

    barrier = pltpu.get_barrier_semaphore()
    peers = [mate]
    for offset in range(cols):
        other = lax.rem(col + offset, cols)
        peers += [{"rows": above, "cols": other}, {"rows": below, "cols": other}]
        if offset:
            peers.append({"cols": other})
    for peer in peers:
        pl.semaphore_signal(barrier, inc=1, device_id=peer, device_id_type=pl.DeviceIdType.MESH)
    pl.semaphore_wait(barrier, len(peers))
    send = Sender(send_sems, recv_sems)

    ham_first = send(ham_ref, ham_v.at[col], side)
    ham_second = send(ham_ref, ham_v.at[col], cross)

    def land(piece, k, part=None):
        size = half if part is None else half // 2
        start = half * space + (0 if part is None else part * size)
        return land_v.at[
            piece // 2,
            piece % 2,
            pl.ds(pl.multiple_of(start, size), size),
            pl.ds(pl.multiple_of(chunk * k, chunk), chunk),
        ]

    order_of_pieces = (0, 2, 1, 3)
    pieces = {}
    for piece in order_of_pieces:
        panel = (1, 2, 1, 0)[piece]
        source = root_ref.at[
            pl.ds(pl.multiple_of(half * space, half), half),
            pl.ds(pl.multiple_of(panel * slab + chunk * col, chunk), chunk),
        ]
        pieces[piece] = send(source, land(piece, col), up if piece < 2 else down)

    zero = jnp.zeros(ortho_v.shape[3:], F32)
    for part in range(2):
        ortho_v[0, 2, part] = zero
        ortho_v[2, 0, part] = zero

    for copy in small:
        copy.wait()
    pattern = pattern_ref[...].astype(F32).astype(BF16)
    blocks_all = pattern.shape[1]

    def pick(rows, block_of):
        wanted = block_of(lax.broadcasted_iota(jnp.int32, (rows, blocks_all), 0))
        here = lax.broadcasted_iota(jnp.int32, (rows, blocks_all), 1)
        chosen = jnp.where(wanted == here, 1.0, 0.0).astype(BF16)
        return lax.dot_general(
            chosen, pattern, (((1,), (1,)), ((), ())), preferred_element_type=F32
        ).astype(BF16)

    def spread(values, wanted):
        here = lax.broadcasted_iota(jnp.int32, wanted.shape, 0)
        return dot(values, jnp.where(wanted == here, 1.0, 0.0).astype(BF16))

    base = row * slab_blocks
    strip_rows = pick(
        cols * own,
        lambda i: base + ((i // own) * 2 + space) * own_blocks + (i % own) // BLK,
    )
    lane = lax.broadcasted_iota(jnp.int32, (3 * slab_blocks, 3 * chunk), 1)
    chip_mask = spread(
        strip_rows, (lane // chunk) * slab_blocks + col * groups + (lane % chunk) // BLK
    )
    for i in range(cols):
        mask_a[i] = chip_mask[i * own : (i + 1) * own]
    own_rows = pick(own, lambda i: base + (col * 2 + space) * own_blocks + i // BLK)
    lane = lax.broadcasted_iota(jnp.int32, (3 * slab_blocks, window), 1)
    mask_b[...] = spread(own_rows, lane // BLK)

    for g in range(own_blocks):
        for p in range(maxb):
            block = pos_ref[g, p]
            within = lax.rem(block, slab_blocks)
            owner = lax.div(within, own_blocks)
            table_s[0, g, p] = lax.div(block, slab_blocks)
            table_s[1, g, p] = lax.rem(owner, 2)
            table_s[2, g, p] = lax.div(owner, 2) * own_blocks + lax.rem(within, own_blocks)
            table_s[3, g, p] = lax.div(within, groups)
            table_s[4, g, p] = lax.rem(within, groups)

    load_root.wait()
    for i in range(cols):
        start = pl.multiple_of((i * 2 + space) * own, own)
        upper, lower = split(root_v[pl.ds(start, own), :])
        left_s[0, i * own : (i + 1) * own] = upper
        left_s[1, i * own : (i + 1) * own] = lower
    for b in range(3):
        wide_hi[1, b], wide_lo[1, b] = split(root_v[:, b * slab : (b + 1) * slab])
        start = pl.multiple_of(b * slab + chunk * col, chunk)
        upper, lower = split(root_v[:, pl.ds(start, chunk)])
        near_hi[1, :, b * chunk : (b + 1) * chunk] = upper
        near_lo[1, :, b * chunk : (b + 1) * chunk] = lower

    relayed = {}
    gathers = {}

    def arrive(piece):
        pieces[piece].wait_recv()
        relayed[piece] = send(land(piece, col), land(piece, col), mate)

    def offer(piece):
        gathers[piece] = [
            send(land(piece, col), land(piece, col), side),
            send(land(piece, col), land(piece, col), cross),
        ]

    def half_rows(k, part):
        return ham_v.at[k, pl.ds(part * (own // 2), own // 2), :]

    arrive(0)
    arrive(2)
    ham_first.wait_recv()
    ham_half_a = send(half_rows(first, 1), half_rows(first, 1), cross)
    ham_second.wait_recv()
    ham_half_b = send(half_rows(second, 0), half_rows(second, 0), side)
    offer(0)
    offer(2)
    arrive(1)
    arrive(3)
    offer(1)
    offer(3)
    for piece in order_of_pieces:
        relayed[piece].wait_recv()
        upper, lower = split(land_v[piece // 2, piece % 2, :, lanes])
        side_of = 0 if piece < 2 else 2
        place = (0, 1, 1, 0)[piece]
        near_hi[side_of, :, place * chunk : (place + 1) * chunk] = upper
        near_lo[side_of, :, place * chunk : (place + 1) * chunk] = lower

    load_ham.wait()
    strips = (col, first, second, third)
    half_up, half_down, half_mate = [], [], []
    for i, strip in enumerate(strips):
        if i == 3:
            ham_half_a.wait_recv()
            ham_half_b.wait_recv()
        stacked = stack(ham_v[strip])
        terms = []
        for a in range(3):
            width = 3 * chunk if a == 1 else 2 * chunk
            terms.append(
                product(
                    stacked[:, a * slab : (a + 1) * slab],
                    (near_hi[a, :, :width], near_lo[a, :, :width]),
                )
            )
        done = mask_a[strip] * combine(*terms, chunk)
        for b in range(3):
            half_v[1, b, strip, space] = done[:, b * chunk : (b + 1) * chunk]
        half_up.append(
            send(
                half_v.at[1, pl.ds(1, 2), strip, space],
                half_v.at[0, pl.ds(0, 2), strip, space],
                up,
            )
        )
        half_down.append(
            send(
                half_v.at[1, pl.ds(0, 2), strip, space],
                half_v.at[2, pl.ds(1, 2), strip, space],
                down,
            )
        )
        half_mate.append(
            send(half_v.at[1, :, strip, space], half_v.at[1, :, strip, space], mate)
        )

    def window_block(ref, a):
        picked = {0: (0, 1), 1: (0, 1, 2), 2: (1, 2)}[a]
        return split(
            jnp.concatenate([ref[a, b].reshape(slab, chunk) for b in picked], axis=1)
        )

    def left_block(a):
        return left_s[:, :, a * slab : (a + 1) * slab].reshape(2 * half, slab)

    for copy in half_mate:
        copy.wait_recv()
    acc_v[...] = product(left_block(1), window_block(half_v, 1))
    relays = []
    mates = []
    for i, piece in enumerate(order_of_pieces):
        half_up[i].wait_recv()
        region = half_v.at[0, pl.ds(0, 2), strips[i], space]
        half_mate.append(send(region, region, mate))
        half_down[i].wait_recv()
        region = half_v.at[2, pl.ds(1, 2), strips[i], space]
        half_mate.append(send(region, region, mate))
        gathers[piece][0].wait_recv()
        relays.append(send(land(piece, first, 1), land(piece, first, 1), cross))
        mates.append(send(land(piece, first), land(piece, first), mate))
        gathers[piece][1].wait_recv()
        relays.append(send(land(piece, second, 0), land(piece, second, 0), side))
        mates.append(send(land(piece, second), land(piece, second), mate))
    for copy in half_mate[cols:]:
        copy.wait_recv()

    done = combine(
        product(left_block(0), window_block(half_v, 0)),
        acc_v[...],
        product(left_block(2), window_block(half_v, 2)),
        chunk,
    )
    for b in range(3):
        masked = mask_a[:, :, b * chunk : (b + 1) * chunk].reshape(half, chunk)
        masked = masked * done[:, b * chunk : (b + 1) * chunk]
        ortho_v[1, b, space, :, col] = masked.reshape(half // BLK, BLK, chunk)

    spans = {0: (0, 2), 1: (0, 3), 2: (1, 2)}

    def region(a, k, b, part=None):
        size = half // BLK if part is None else half // BLK // 2
        start = 0 if part is None else part * size
        return ortho_v.at[a, b, space, pl.ds(start, size), k]

    def pass_on(a, k, b, part, device):
        return send(region(a, k, b, part), region(a, k, b, part), device)

    def to_rows(k, b, part):
        copies = []
        if b > 0:
            copies.append((0, b - 1, send(region(1, k, b, part), region(0, k, b - 1, part), up)))
        if b < 2:
            copies.append((2, b + 1, send(region(1, k, b, part), region(2, k, b + 1, part), down)))
        return copies

    panels = (1, 0, 2)
    pending = []
    own_rows_out, own_first, own_second = {}, {}, {}
    for b in panels:
        own_rows_out[b] = to_rows(col, b, None)
        own_first[b] = pass_on(1, col, b, None, side)
        own_second[b] = pass_on(1, col, b, None, cross)
        pending.append(pass_on(1, col, b, None, mate))
    for copy in relays:
        copy.wait_recv()
    for piece in order_of_pieces:
        mates.append(send(land(piece, third), land(piece, third), mate))
    for copy in mates:
        copy.wait_recv()
    for piece in order_of_pieces:
        a = 0 if piece < 2 else 2
        b = (0, 1, 2, 1)[piece]
        wide_hi[a, b], wide_lo[a, b] = split(land_v[piece // 2, piece % 2])

    hops, diagonals, first_rows, second_rows = [], {}, {}, {}
    for b in panels:
        own_first[b].wait_recv()
        first_rows[b] = to_rows(first, b, 0)
        diagonal_a = pass_on(1, first, b, 1, cross)
        pending.append(pass_on(1, first, b, None, mate))
        own_second[b].wait_recv()
        second_rows[b] = to_rows(second, b, 1)
        diagonals[b] = (diagonal_a, pass_on(1, second, b, 0, side))
        pending.append(pass_on(1, second, b, None, mate))
        for a, place, copy in own_rows_out[b]:
            copy.wait_recv()
            hops.append((a, first, place, 1, pass_on(a, col, place, 1, side)))
            hops.append((a, second, place, 0, pass_on(a, col, place, 0, cross)))
            pending.append(pass_on(a, col, place, None, mate))
    for b in panels:
        for copy in diagonals[b]:
            copy.wait_recv()
        pending.append(pass_on(1, third, b, None, mate))
        for a, place, copy in first_rows[b]:
            copy.wait_recv()
            hops.append((a, third, place, 0, pass_on(a, first, place, 0, cross)))
            pending.append(pass_on(a, first, place, 0, mate))
        for a, place, copy in second_rows[b]:
            copy.wait_recv()
            hops.append((a, third, place, 1, pass_on(a, second, place, 1, side)))
            pending.append(pass_on(a, second, place, 1, mate))
    for a, k, place, part, copy in hops:
        copy.wait_recv()
        pending.append(pass_on(a, k, place, part, mate))
    for copy in pending:
        copy.wait_recv()

    lane_group = lax.broadcasted_iota(jnp.int32, (8, chunk), 1) // BLK

    def solve(g):
        live = count_ref[g]

        for p in range(maxb):
            sub = table_s[4, g, p]
            steps = lax.rem(p + groups - sub, groups)
            turns_v[p] = jnp.where(
                lane_group == jnp.full(lane_group.shape, sub, jnp.int32),
                jnp.full(lane_group.shape, steps, jnp.int32),
                -1,
            )

        def assemble(i, inner):
            a, core, place = (table_s[field, g, i] for field in range(3))
            for t in range(maxb // groups):
                sorted_by = [jnp.zeros((BLK, chunk), F32)] * groups
                for e in range(groups):
                    p = t * groups + e
                    value = ortho_v[a, table_s[0, g, p], core, place, table_s[3, g, p]]
                    needed = jnp.tile(turns_v[p], (BLK // 8, 1))
                    for steps in range(groups):
                        sorted_by[steps] = jnp.where(needed == steps, value, sorted_by[steps])
                tile = sorted_by[0]
                for steps in range(1, groups):
                    tile = tile + pltpu.roll(sorted_by[steps], steps * BLK, 1)
                sub_v[pl.ds(pl.multiple_of(i * BLK, BLK), BLK), t * chunk : (t + 1) * chunk] = tile
            return inner

        lax.fori_loop(0, maxb, assemble, 0, unroll=2)
        position = [lax.broadcasted_iota(jnp.int32, (order, order), d) for d in range(2)]
        assembled = jnp.where(jnp.maximum(*position) < live * BLK, sub_v[...], 0.0)
        symmetric = 0.5 * (assembled + assembled.T)
        total = jnp.sum(jnp.sum(symmetric * symmetric, axis=1, keepdims=True), axis=0, keepdims=True)
        live_order = jnp.full((1, 1), live * BLK, jnp.int32).astype(F32)
        iterate = symmetric * (jnp.sqrt(live_order) / (2.0 * jnp.sqrt(total + 1e-06)))
        parts = split(iterate)
        square = split(dot(parts[0], parts[0]) + dot(parts[0], parts[1]) + dot(parts[1], parts[0]))

        def times_square(value):
            return product(stack(value), square)

        home = iterate[:BLK]
        home = 1.5 * home - 0.5 * times_square(home)
        cube = times_square(home)
        cube = 1.5 * cube - 0.5 * times_square(cube)
        cube = 1.5 * cube - 0.5 * times_square(cube)
        home = 1.5 * home - 0.5 * cube
        diagonal = lax.broadcasted_iota(jnp.int32, (BLK, order), 0) == lax.broadcasted_iota(
            jnp.int32, (BLK, order), 1
        )
        home = 0.5 * (jnp.where(diagonal, 1.0, 0.0) - home)
        tiles = [jnp.zeros((BLK, chunk), F32) for _ in range(window // chunk)]
        turned = [
            [home[:, t * chunk : (t + 1) * chunk]]
            + [
                pltpu.roll(home[:, t * chunk : (t + 1) * chunk], steps * BLK, 1)
                for steps in range(1, groups)
            ]
            for t in range(maxb // groups)
        ]
        for p in range(maxb):
            other = pos_ref[g, p]
            sub = lax.rem(other, groups)
            here = (lane_group == jnp.full(lane_group.shape, sub, jnp.int32)) & (
                jnp.full(lane_group.shape, live, jnp.int32) > p
            )
            place = jnp.where(
                here, jnp.full(lane_group.shape, lax.div(other, groups), jnp.int32), -1
            )
            place = jnp.tile(place, (BLK // 8, 1))
            ways = turned[p // groups]
            wide = jnp.tile(lane_group, (BLK // 8, 1))
            value = ways[(groups - p) % groups]
            for target in range(1, groups):
                value = jnp.where(wide == target, ways[(target + groups - p) % groups], value)
            for m in range(len(tiles)):
                tiles[m] = jnp.where(place == m, value, tiles[m])
        return jnp.concatenate(tiles, axis=1)

    def lanes_of(k):
        return pl.ds(pl.multiple_of(chunk * k, chunk), chunk)

    back_mate = []
    back = {
        (a, g, offset): []
        for a in (1, 0, 2)
        for g in range(own_blocks)
        for offset in (2, 1, 3, 0)
        if a != 1 or offset
    }
    for g in range(own_blocks):
        stacked = stack(solve(g))
        these = pl.ds(g * BLK, BLK)
        for b in (1, 0, 2):
            total = None
            for a in (0, 1, 2):
                if abs(a - b) > 1:
                    continue
                term = product(
                    stacked[:, a * slab : (a + 1) * slab], (wide_hi[a, b], wide_lo[a, b])
                )
                total = term if total is None else total + term
            rows_v[b, these] = mask_b[these, b * slab : (b + 1) * slab] * total
            for offset in (2, 1, 3, 0):
                target = lax.rem(col + offset, cols)
                source = rows_v.at[b, these, lanes_of(target)]
                if b > 0:
                    target_ref = back_v.at[0, b - 1, col, space, these]
                    device = {"rows": above, "cols": target}
                    back[0, g, offset].append(send(source, target_ref, device))
                if b < 2:
                    target_ref = back_v.at[2, b + 1, col, space, these]
                    device = {"rows": below, "cols": target}
                    back[2, g, offset].append(send(source, target_ref, device))
            for offset in (2, 1, 3):
                target = lax.rem(col + offset, cols)
                source = rows_v.at[b, these, lanes_of(target)]
                target_ref = back_v.at[1, b, col, space, these]
                back[1, g, offset].append(send(source, target_ref, {"cols": target}))
        back_mate.append(
            send(rows_v.at[:, these, lanes], back_v.at[1, :, col, space, these], mate)
        )
    back_v[1, :, col, space] = rows_v[:, :, lanes]
    for (a, g, offset), copies in sorted(
        back.items(), key=lambda item: (item[0][0] != 1, item[0][1])
    ):
        for copy in copies:
            copy.wait_recv()
        origin = lax.rem(col + cols - offset, cols)
        piece = back_v.at[a, pl.ds(*spans[a]), origin, space, pl.ds(g * BLK, BLK)]
        back_mate.append(send(piece, piece, mate))
        if len(back_mate) == own_blocks * cols:
            for other in back_mate:
                other.wait_recv()
            acc_v[...] = product(left_block(1), window_block(back_v, 1))
    for other in back_mate[own_blocks * cols :]:
        other.wait_recv()
    outer = [window_block(back_v, a) for a in (0, 2)]
    outs = []
    for offset in (2, 1, 3, 0):
        target = lax.rem(col + offset, cols)
        rows = pl.ds(pl.multiple_of(target * own, own), own)
        terms = [
            product(left_s[:, rows, a * slab : (a + 1) * slab].reshape(2 * own, slab), right)
            for a, right in zip((0, 2), outer)
        ]
        done = mask_a[target] * combine(terms[0], acc_v[rows, :], terms[1], chunk)
        for b in range(3):
            strip_v[target, b] = done[:, b * chunk : (b + 1) * chunk]
        if offset:
            outs.append(send(strip_v.at[target], final_v.at[col], {"cols": target}))
    final_v[col] = strip_v[col]
    for copy in outs:
        copy.wait_recv()
    total = jnp.zeros((own, chunk), F32)
    for b in range(3):
        for k in range(cols):
            value = final_v[k, b]
            total = total + value
            density_ref[:, b * slab + k * chunk : b * slab + (k + 1) * chunk] = value
    charges_ref[...] = jnp.sum(total.T, axis=0)
    send.finish()


def place_kernel(density_ref, charges_ref, density_out, charges_out, density_v, charges_v, sems):
    inward = [
        pltpu.make_async_copy(density_ref, density_v, sems.at[0]),
        pltpu.make_async_copy(charges_ref, charges_v, sems.at[1]),
    ]
    outward = [
        pltpu.make_async_copy(density_v, density_out, sems.at[2]),
        pltpu.make_async_copy(charges_v, charges_out, sems.at[3]),
    ]
    for copy in inward:
        copy.start()
    for copy, then in zip(inward, outward):
        copy.wait()
        then.start()
    for copy in outward:
        copy.wait()


def shards(hamiltonian, correlation_root, pattern, sub_blocks, sub_count):
    slab, window = correlation_root.shape
    own = hamiltonian.shape[0]
    cols = lax.axis_size("cols")
    chunk = slab // cols
    half = slab // 2
    own_blocks, maxb = sub_blocks.shape
    order = maxb * BLK
    vmem = functools.partial(pltpu.VMEM)
    density, charges = pl.pallas_call(
        kernel,
        out_shape=[
            jax.ShapeDtypeStruct((own, window), F32),
            jax.ShapeDtypeStruct((own,), F32),
        ],
        in_specs=[
            pl.BlockSpec(memory_space=pltpu.HBM),
        ]
        * 5,
        out_specs=[pl.BlockSpec(memory_space=pltpu.VMEM)] * 2,
        scratch_shapes=[
            vmem((slab, window), F32),
            vmem((2, half, window), BF16),
            vmem((cols, own, window), F32),
            vmem((2, 2, slab, slab), F32),
            vmem((3, 3, slab, slab), BF16),
            vmem((3, 3, slab, slab), BF16),
            vmem((3, slab, 3 * chunk), BF16),
            vmem((3, slab, 3 * chunk), BF16),
            vmem((cols, own, 3 * chunk), F32),
            vmem((own, window), F32),
            vmem((3, 3, cols, 2, own, chunk), F32),
            vmem((3, 3, cols, 2, own, chunk), F32),
            vmem((3, 3, 2, half // BLK, cols, BLK, chunk), F32),
            vmem((half, 3 * chunk), F32),
            vmem((order, order), F32),
            vmem((maxb, 8, chunk), jnp.int32),
            vmem((3, own, slab), F32),
            vmem((cols, 3, own, chunk), F32),
            vmem((cols, 3, own, chunk), F32),
            pltpu.VMEM(pattern.T.shape, jnp.int32),
            pltpu.SMEM(sub_blocks.shape, jnp.int32),
            pltpu.SMEM(sub_count.shape, jnp.int32),
            pltpu.SMEM((5, own_blocks, maxb), jnp.int32),
            pltpu.SemaphoreType.DMA((5,)),
            pltpu.SemaphoreType.DMA((320,)),
            pltpu.SemaphoreType.DMA((320,)),
        ],
        compiler_params=pltpu.CompilerParams(
            collective_id=1, has_side_effects=True, vmem_limit_bytes=62 * 2**20
        ),
    )(sub_blocks, sub_count, hamiltonian, correlation_root, pattern.T)
    return pl.pallas_call(
        place_kernel,
        out_shape=[
            jax.ShapeDtypeStruct((own, window), F32),
            jax.ShapeDtypeStruct((own,), F32),
        ],
        in_specs=[pl.BlockSpec(memory_space=pltpu.HBM)] * 2,
        out_specs=[pl.BlockSpec(memory_space=pltpu.HBM)] * 2,
        scratch_shapes=[
            pltpu.VMEM((own, window), F32),
            pltpu.VMEM((own,), F32),
            pltpu.SemaphoreType.DMA((4,)),
        ],
        compiler_params=pltpu.CompilerParams(vmem_limit_bytes=62 * 2**20),
    )(density, charges)


def solution(mesh):
    return jax.shard_map(
        shards,
        mesh=mesh,
        in_specs=(
            P(("rows", "cols", "space"), None),
            P("rows", None),
            P(),
            P(("rows", "cols", "space"), None),
            P(("rows", "cols", "space")),
        ),
        out_specs=(P(("rows", "cols", "space"), None), P(("rows", "cols", "space"))),
        check_vma=False,
    )
```
